32 devices in a mesh: expert: 16 (over z, y, core), replica: 2 (over x).
Axes of the slice: x: 2, y: 2, z: 4, core: 2. Of those that a mesh axis runs over, the one named last changes fastest.
Arguments:
- tokens: bfloat16 [4096, 2048], P(('expert', 'replica')), may hold values from -15 to 15
- cotangents: bfloat16 [4096, 768], P(('expert', 'replica')), may hold values from -6 to 6
- routes: int32 [4096, 8], P(('expert', 'replica')), may hold values from 0 to 127, all different within a row; in each aligned block of 128 rows (0 to 127, 128 to 255, ...) at most 12 rows name the same one
- owner: int32 [16], P('expert'), may hold values from 0 to 1
- a_inverse: bfloat16 [16, 2048, 2048], P('expert', 'replica'), may hold values from -1 to 33, as said below
- g_inverse: bfloat16 [16, 768, 768], P('expert'), may hold values from -1 to 33
Outputs:
- a_factor: float32 [16, 2048, 2048], P('expert', 'replica')
- kept_factor: float32 [2, 16, 768, 768], P('replica', 'expert')
- update: bfloat16 [16, 2048, 768], P('expert')
The draws below stay inside these ranges and needn't reach their ends.
Inputs may be any that keep to these rules, and one draw needn't show every extreme that they name: `routes`: the 8 ids of a row differ; among the rows of one device no id occurs more than 12 times and some id occurs exactly 12 times; every id occurs somewhere. Each a_inverse[v] is symmetric.
All inputs are finite; a program needn't handle non-finite values.
Results may differ from the reference program's by a relative error of at most 0.018.
Values may be sent and summed in bfloat16 or wider, within the bound.
No kernel may reach another device: no remote copies, remote signals or barrier semaphores. Data moves between devices by JAX's collectives and lax.ppermute only.
A program may use at most 128 MiB of HBM per device.

```python
import math
import jax
import jax.numpy as jnp
import numpy as np
from jax import lax

D = 2048
HID = 768
ALL_EXPERTS = 128
TOP = 8
TOK_DEV = 128
CAP = 12
EXPERTS = 16
TOKENS = 4096
N_EXPERT = 16
N_REPLICA = 2


def inverse_like(key, count, width):
    first, second = jax.random.split(key)
    low_end, high_end = (4.0, 16.0)
    diagonal = jnp.exp(jax.random.uniform(first, (count, width), jnp.float32, math.log(low_end), math.log(high_end)))
    noise = jax.random.truncated_normal(second, -4.0, 4.0, (count, width, width), jnp.float32) * (2.2 / math.sqrt(width))
    symmetric = (noise + jnp.swapaxes(noise, 1, 2)) * (1.0 / math.sqrt(2.0))
    symmetric = jnp.clip(symmetric, -1.0, 1.0)
    return symmetric + diagonal[:, :, None] * jnp.eye(width, dtype=jnp.float32)[None]


def draw_a_inverse(key, part):
    return inverse_like(jax.random.fold_in(key, 11), EXPERTS, D).astype(jnp.bfloat16)


def draw_g_inverse(key, part):
    return inverse_like(jax.random.fold_in(key, 23), EXPERTS, HID).astype(jnp.bfloat16)


def draw_tokens(key, part):
    first, second = jax.random.split(jax.random.fold_in(key, 37), 2)
    feature_scale = jnp.exp(jax.random.uniform(first, (D,), jnp.float32, math.log(0.3), math.log(3.0)))
    values = jax.random.truncated_normal(second, -5.0, 5.0, (TOKENS, D), jnp.float32)
    return (values * feature_scale[None, :]).astype(jnp.bfloat16)


def set_ends(array, own_key, smallest, largest):
    spot = [jax.random.randint(jax.random.fold_in(own_key, axis), (), 0, length) for axis, length in enumerate(array.shape)]
    main_axis = array.shape.index(max(array.shape))
    neighbour = spot[:main_axis] + [(spot[main_axis] + 1) % array.shape[main_axis]] + spot[main_axis + 1:]
    return array.at[tuple(spot)].set(smallest).at[tuple(neighbour)].set(largest)


def steps_of(key, extent, cuts, low, top_value):
    gain = 1.0
    for dim, parts in cuts:
        steps = jax.random.uniform(jax.random.fold_in(jax.random.fold_in(key, 6), dim), (parts,), jnp.float32, low / len(cuts), top_value / len(cuts))
        gain = gain * jnp.repeat(jnp.exp(steps), extent[dim] // parts).reshape((-1,) + (1,) * (len(extent) - 1 - dim))
    return gain


def shared_out(key, own, number, rows, amount, top, limit, skew):
    sequence = jax.random.permutation(key, amount)
    crowded, common = shares(amount, rows * top, limit, skew, True), shares(amount, rows * top, limit, skew, False)
    places = jnp.arange(amount)

    def named(sizes, offset_by):
        used = int((sizes > 0).sum())
        fixed = max(1, used // 4)
        passed = fixed + (places - fixed + offset_by * (used - fixed)) % max(1, amount - fixed)
        return jnp.zeros((amount,), jnp.int32).at[sequence[jnp.where(places < fixed, places, passed)]].set(jnp.asarray(sizes, jnp.int32))

    sizes = jnp.where(number % 4 == 0, named(crowded, number // 4), named(common, number - number // 4 - 1))
    mixed = jax.random.permutation(jax.random.fold_in(own, 3), amount)
    giver, sink = mixed[0:amount // 2 * 2:2], mixed[1:amount // 2 * 2:2]
    slack = jnp.minimum(sizes[giver] - 1, limit - sizes[sink]) // 2
    slack = jnp.where((giver == sequence[0]) | (sink == sequence[0]) | (sizes[sink] == 0), 0, jnp.maximum(slack, 0))
    passed = jax.random.randint(jax.random.fold_in(own, 4), (amount // 2,), 0, 1 << 20) % (slack + 1)
    sizes = sizes.at[giver].add(-passed).at[sink].add(passed)
    items = jnp.searchsorted(jnp.cumsum(sizes), jnp.arange(rows * top), side="right").astype(jnp.int32)
    table = items.reshape(top, rows).T
    table = table[jax.random.permutation(jax.random.fold_in(own, 1), rows)]
    offset_by = jax.random.randint(jax.random.fold_in(own, 2), (rows, 1), 0, top)
    return jnp.take_along_axis(table, (jnp.arange(top)[None, :] + offset_by) % top, axis=1)


def shares(count, total, limit, slope, full):
    portions = [(1 << 20) // math.isqrt(rank ** slope) + 1 for rank in range(1, count + 1)]
    largest = limit if full else min(limit, max(-(-total // count), total * portions[0] // sum(portions)))
    least = 1 if total - largest >= count - 1 else 0
    given, surplus = [largest] + [least] * (count - 1), total - largest - least * (count - 1)
    while surplus > 0:
        free = [i for i in range(1, count) if given[i] < largest] or [i for i in range(1, count) if given[i] < limit]
        whole, budget = sum([portions[i] for i in free]), surplus
        for i in free:
            addition = min(limit - given[i], max(1, budget * portions[i] // whole), surplus)
            given[i] = given[i] + addition
            surplus = surplus - addition
    return np.array(given)


def gaussian(stream_key, dims, scale, reach, pieces=(), kind=jnp.bfloat16):
    result = jax.random.normal(stream_key, dims, jnp.float32) * scale
    if len(pieces) > 0:
        result = steps_of(stream_key, dims, pieces, -0.22, 0.18) * result
    return jnp.clip(result, min=-reach, max=reach).astype(kind)


def setup_inputs(seed: int = 0) -> dict:
    key_list = jax.random.split(jax.random.key(seed), 7)
    tokens = draw_tokens(jax.random.fold_in(key_list[6], 71), 0)
    cotangents = gaussian(key_list[1], (TOKENS, HID), 1.0, 6.0, ((0, 32),))
    routes_keys = jax.random.split(jax.random.fold_in(key_list[2], 1), TOKENS // TOK_DEV)
    routes_turns = jax.random.permutation(jax.random.fold_in(key_list[2], 3), TOKENS // TOK_DEV)
    routes = jax.vmap(lambda own, number: shared_out(jax.random.fold_in(key_list[2], 2), own, number, TOK_DEV, ALL_EXPERTS, TOP, CAP, 2))(routes_keys, routes_turns).reshape((TOKENS, TOP))
    owner = set_ends(jax.random.randint(key_list[3], (EXPERTS,), 0, N_REPLICA), jax.random.fold_in(key_list[3], 1), 0, N_REPLICA - 1).astype(jnp.int32)
    a_inverse = draw_a_inverse(jax.random.fold_in(key_list[6], 71), 0)
    g_inverse = draw_g_inverse(jax.random.fold_in(key_list[6], 71), 0)
    return dict(tokens=tokens, cotangents=cotangents, routes=routes, owner=owner, a_inverse=a_inverse, g_inverse=g_inverse)


def slot_table(route_block, expert_count, capacity):
    top_k = route_block.shape[1]
    route_ids = route_block.reshape(-1).astype(jnp.int32)
    in_window = route_ids < expert_count
    columns = lax.broadcasted_iota(jnp.int32, (route_ids.shape[0], expert_count), 1)
    one_hot = ((route_ids[:, None] == columns) & in_window[:, None]).astype(jnp.int32)
    before = jnp.cumsum(one_hot, axis=0) - one_hot
    position = jnp.sum(before * one_hot, axis=1).astype(jnp.int32)
    sentinel = expert_count * capacity
    slot_ids = jnp.where(in_window, route_ids * capacity + position, sentinel).astype(jnp.int32)
    source_ids = (jnp.arange(route_ids.shape[0], dtype=jnp.int32) // top_k).astype(jnp.int32)
    slot_token = jnp.zeros((sentinel + 1,), jnp.int32).at[slot_ids].set(source_ids)
    filled = jnp.zeros((sentinel + 1,), jnp.int32).at[slot_ids].set(1)
    return slot_token[:sentinel], filled[:sentinel]


def device_buffers(token_block, cotangent_block, route_block):
    slot_token, filled = slot_table(route_block, N_EXPERT, CAP)
    slot_mask = filled.astype(token_block.dtype)[:, None]
    send_x = (jnp.take(token_block, slot_token, axis=0) * slot_mask).reshape(N_EXPERT, CAP, D)
    send_y = (jnp.take(cotangent_block, slot_token, axis=0) * slot_mask).reshape(N_EXPERT, CAP, HID)
    return send_x, send_y, filled.reshape(N_EXPERT, CAP)


def reference(tokens, cotangents, routes, owner, a_inverse, g_inverse):
    devices = N_EXPERT * N_REPLICA
    send_x, send_y, filled = jax.vmap(device_buffers)(
        tokens.reshape(devices, TOK_DEV, D),
        cotangents.reshape(devices, TOK_DEV, HID),
        routes.reshape(devices, TOK_DEV, TOP))

    def one_expert(index):
        block_x = send_x[:, index]
        block_y = send_y[:, index]
        routed = jnp.sum(filled[:, index]).astype(jnp.float32)
        rows_x = block_x.reshape(-1, D)
        a_full = jnp.dot(rows_x.T, rows_x, preferred_element_type=jnp.float32) / routed
        by_replica_x = block_x.reshape(N_EXPERT, N_REPLICA, CAP, D).transpose(1, 0, 2, 3).reshape(N_REPLICA, N_EXPERT * CAP, D)
        by_replica_y = block_y.reshape(N_EXPERT, N_REPLICA, CAP, HID).transpose(1, 0, 2, 3).reshape(N_REPLICA, N_EXPERT * CAP, HID)
        wide_x = by_replica_x.astype(jnp.float32)
        wide_y = by_replica_y.astype(jnp.float32)
        g_parts = jnp.einsum('rnh,rng->rhg', wide_y, wide_y).astype(jnp.bfloat16)
        g_parts = lax.optimization_barrier(g_parts).astype(jnp.float32)
        g_sum = jnp.sum(g_parts, axis=0)
        w_parts = jnp.einsum('rnd,rnh->rdh', wide_x, wide_y).astype(jnp.bfloat16)
        w_parts = lax.optimization_barrier(w_parts).astype(jnp.float32)
        grad = (jnp.sum(w_parts, axis=0) / routed).astype(jnp.bfloat16)
        mixed = jnp.dot(a_inverse[index], grad, preferred_element_type=jnp.float32).astype(jnp.bfloat16)
        update = jnp.dot(mixed, g_inverse[index], preferred_element_type=jnp.float32).astype(jnp.bfloat16)
        replica_ids = jnp.arange(N_REPLICA, dtype=jnp.int32)[:, None, None]
        kept = jnp.where(replica_ids == owner[index], (g_sum / routed)[None], jnp.zeros((1, HID, HID), jnp.float32))
        return a_full, kept, update

    a_factor, kept, update = lax.map(one_expert, jnp.arange(N_EXPERT, dtype=jnp.int32))
    return a_factor, kept.transpose(1, 0, 2, 3), update
```

```python
import functools

import jax
import jax.numpy as jnp
from jax import lax
from jax.experimental import pallas as pl
from jax.experimental.pallas import tpu as pltpu
from jax.sharding import PartitionSpec as P

CAP = 12
MAIN = 8
EMPTY = 1024.0


F32 = jnp.float32
BF16 = jnp.bfloat16
VMEM = pl.BlockSpec(memory_space=pltpu.VMEM)
SMEM = pl.BlockSpec(memory_space=pltpu.SMEM)
ANY = pl.BlockSpec(memory_space=pl.ANY)


def dot(a, b):
    return jnp.dot(a, b, preferred_element_type=F32)


def dot_nt(a, b):
    return lax.dot_general(a, b, (((1,), (1,)), ((), ())), preferred_element_type=F32)


def dot_tn(a, b):
    return lax.dot_general(a, b, (((0,), (0,)), ((), ())), preferred_element_type=F32)


def pack_kernel(me_ref, routes_ref, x_ref, y_ref, *out_refs):
    me = me_ref[0]
    top, toks = routes_ref.shape
    width, hidden = x_ref.shape[1], y_ref.shape[1]
    half = (width + hidden) // 2
    rows = len(out_refs) * MAIN
    row = lax.broadcasted_iota(jnp.int32, (rows, toks), 0)
    ids = (row // MAIN) ^ me
    chosen = jnp.zeros((rows, toks), F32)
    for k in range(top):
        chosen += jnp.where(routes_ref[k : k + 1, :] == ids, 1.0, 0.0)
    earlier = lax.broadcasted_iota(jnp.int32, (toks, toks), 0) < lax.broadcasted_iota(
        jnp.int32, (toks, toks), 1
    )
    before = dot(chosen.astype(BF16), jnp.where(earlier, 1.0, 0.0).astype(BF16))
    slot = jnp.where(chosen > 0.0, before, -1.0).astype(jnp.int32)
    sub = row % MAIN
    low = sub < MAIN // 2
    pick = jnp.where(slot == sub, 1.0, 0.0)
    rest = jnp.where(slot == jnp.where(low, MAIN + sub, MAIN // 2 + sub), 1.0, 0.0)
    free = jnp.sum(pick, axis=1, keepdims=True) == 0.0
    free_rest = jnp.sum(rest, axis=1, keepdims=True) == 0.0
    pick_b = pick.astype(BF16)
    lo_b = jnp.where(low, rest, 0.0).astype(BF16)
    hi_b = jnp.where(low, 0.0, rest).astype(BF16)
    lane0 = lax.broadcasted_iota(jnp.int32, (rows, 128), 1) == 0
    low_lanes = lax.broadcasted_iota(jnp.int32, (rows, 128), 0) % MAIN < MAIN // 2

    def put(at, value):
        for k, ref in enumerate(out_refs):
            ref[:, at : at + value.shape[1]] = value[k * MAIN : (k + 1) * MAIN].astype(BF16)

    first = dot(pick_b, x_ref[:, :128])
    put(0, jnp.where(lane0 & free, EMPTY, first))
    put(128, dot(pick_b, x_ref[:, 128:]))
    put(width, dot(pick_b, y_ref[...]))
    base = width + hidden
    split = width - half
    rem = dot(lo_b, x_ref[:, :split]) + dot(hi_b, x_ref[:, half:])
    put(base, jnp.where(lane0 & low_lanes & free_rest, EMPTY, rem[:, :128]))
    put(base + 128, rem[:, 128:])
    put(base + split, dot(lo_b, x_ref[:, split:half]) + dot(hi_b, y_ref[...]))


def pack(me, routes, tokens, cotangents, blocks):
    width = (tokens.shape[1] + cotangents.shape[1]) * CAP // MAIN
    return pl.pallas_call(
        pack_kernel,
        name="pack",
        out_shape=[jax.ShapeDtypeStruct((MAIN, width), BF16)] * blocks,
        in_specs=[SMEM, VMEM, VMEM, VMEM],
        out_specs=[VMEM] * blocks,
        cost_estimate=pl.CostEstimate(
            flops=2 * blocks * MAIN * tokens.shape[0] * width, bytes_accessed=2**21, transcendentals=0
        ),
    )(me, routes.T, tokens, cotangents)


def fold_kernel(rep_ref, a_ref, tri_ref, square_ref):
    half = square_ref.shape[0]
    p, s = a_ref[0, :half, :half], a_ref[0, half:, half:]
    row = lax.broadcasted_iota(jnp.int32, (half, half), 0)
    col = lax.broadcasted_iota(jnp.int32, (half, half), 1)
    tri_ref[:half, :] = jnp.where(col >= row, p.astype(F32), s.astype(F32)).astype(BF16)
    diagonal = jnp.sum(jnp.where(row == col, s.astype(F32), 0.0), axis=0, keepdims=True)
    tri_ref[half:, :] = jnp.broadcast_to(diagonal, (16, half)).astype(BF16)
    square_ref[...] = a_ref[0, :half, half:]


def fold(rep, a_inverse):
    side = a_inverse.shape[1]
    half = side // 2
    return pl.pallas_call(
        fold_kernel,
        name="fold",
        out_shape=[
            jax.ShapeDtypeStruct((half + 16, half), BF16),
            jax.ShapeDtypeStruct((half, half), BF16),
        ],
        grid_spec=pltpu.PrefetchScalarGridSpec(
            num_scalar_prefetch=1,
            grid=(1,),
            in_specs=[pl.BlockSpec((1, side, side), lambda i, rep: (0, 0, rep[0]))],
            out_specs=[
                pl.BlockSpec((half + 16, half), lambda i, rep: (0, 0)),
                pl.BlockSpec((half, half), lambda i, rep: (0, 0)),
            ],
        ),
        cost_estimate=pl.CostEstimate(flops=side * side, bytes_accessed=3 * side * side, transcendentals=0),
    )(rep, a_inverse)


def gather_rows(groups, x_ref, y_ref):
    cols = x_ref.shape[2]
    width = 2 * cols
    hidden = y_ref.shape[1]
    half = (width + hidden) // 2
    base = width + hidden
    at = 0
    for ref in groups:
        count = ref.shape[0]
        x_ref[0, at : at + count, :] = ref[:, :cols]
        x_ref[1, at : at + count, :] = ref[:, cols:width]
        y_ref[at : at + count, :] = ref[:, width:base]
        at += count
    for first, second in zip(groups[::2], groups[1::2]):
        count = first.shape[0]
        low = lax.broadcasted_iota(jnp.int32, (count, half), 0) % MAIN < MAIN // 2
        one, two = first[:, base:].astype(F32), second[:, base:].astype(F32)
        lo = jnp.where(low, one, pltpu.roll(two, MAIN // 2, 0)).astype(BF16)
        hi = jnp.where(low, pltpu.roll(one, count - MAIN // 2, 0), two).astype(BF16)
        x_ref[0, at : at + count, :] = lo[:, :cols]
        x_ref[1, at : at + count, : half - cols] = lo[:, cols:]
        x_ref[1, at : at + count, half - cols :] = hi[:, : width - half]
        y_ref[at : at + count, :] = hi[:, width - half :]
        at += count
    edge = x_ref[0, :, :128].astype(F32)
    empty = (lax.broadcasted_iota(jnp.int32, edge.shape, 1) == 0) & (edge == EMPTY)
    x_ref[0, :, :128] = jnp.where(empty, 0.0, edge).astype(BF16)
    return at - jnp.sum(jnp.where(empty, 1.0, 0.0))


def main_kernel(
    rep_ref,
    owner_ref,
    near_ref,
    far_ref,
    near2_ref,
    far2_ref,
    tri_ref,
    g_ref,
    a_hbm,
    a_out,
    kept_ref,
    u_out,
    part_ref,
    x_ref,
    v_ref,
    inv_ref,
    y_ref,
    a_ref,
    ps_ref,
    abuf,
    ubuf,
    in_sem,
    a_sem,
    u_sem,
):
    rep = rep_ref[0]
    oth = 1 - rep
    side = a_ref.shape[1]
    half = side // 2
    loads = [
        pltpu.make_async_copy(a_hbm.at[0, :, pl.ds(h * side, side)], a_ref.at[h], in_sem.at[h])
        for h in range(2)
    ]
    for load in loads:
        load.start()
    count = gather_rows([near_ref, far_ref, near2_ref, far2_ref], x_ref, y_ref)
    inv = 1.0 / jnp.full((8, 128), count, F32)
    inv_ref[...] = inv
    inv = inv[:1, :1]

    step = abuf.shape[1]
    writes = []
    for i in range(side // step):
        slot = i % 2
        if i >= 2:
            writes[i - 2].wait()
        lhs = x_ref[rep, :, i * step : (i + 1) * step]
        for h in range(2):
            abuf[slot, :, h * side : (h + 1) * side] = dot_tn(lhs, x_ref[h]) * inv
        write = pltpu.make_async_copy(abuf.at[slot], a_out.at[0, pl.ds(i * step, step), :], a_sem.at[slot])
        write.start()
        writes.append(write)

    v_ref[...] = dot(y_ref[...], g_ref[0]).astype(BF16)
    keep = jnp.where(owner_ref[0] == rep, 1.0, 0.0) * inv
    kept_ref[0, 0] = dot_tn(y_ref[...], y_ref[...]) * keep

    for load in loads:
        load.wait()
    tile = 256
    stores = []
    for c in range(side // tile):
        cols = slice(c * tile, (c + 1) * tile)
        mixed = dot(x_ref[rep], a_ref[rep, :, cols]) + dot_nt(x_ref[oth], a_ref[oth, cols, :])
        ubuf[cols, :] = (dot_tn(mixed.astype(BF16), v_ref[...]) * inv).astype(BF16)
        store = pltpu.make_async_copy(
            ubuf.at[pl.ds(c * tile, tile)], u_out.at[0, pl.ds(rep * side + c * tile, tile), :], u_sem.at[c]
        )
        store.start()
        stores.append(store)
    mix = tri_ref[:half, :].astype(F32)
    mix_t = mix.T
    row = lax.broadcasted_iota(jnp.int32, (half, half), 0)
    col = lax.broadcasted_iota(jnp.int32, (half, half), 1)
    diagonal = tri_ref[half : half + 1, :].astype(F32)
    ps_ref[0] = jnp.where(col >= row, mix, mix_t).astype(BF16)
    ps_ref[1] = jnp.where(col < row, mix, jnp.where(col == row, diagonal, mix_t)).astype(BF16)
    for c in range(side // tile):
        cols = slice(c * tile, (c + 1) * tile)
        h, inner = divmod(c * tile, half)
        part_ref[:, cols] = dot(x_ref[rep], a_ref[oth, :, cols]) + dot(
            x_ref[oth, :, h * half : (h + 1) * half], ps_ref[h, :, inner : inner + tile]
        )
    writes[-2].wait()
    writes[-1].wait()
    for store in stores:
        store.wait()


def products(rep, owner, groups, tri, g_inverse, a_inverse):
    rows = sum(g.shape[0] for g in groups) * CAP // MAIN
    _, side, width = a_inverse.shape
    hidden = g_inverse.shape[1]
    half = side // 2
    step = 256
    return pl.pallas_call(
        main_kernel,
        name="products",
        out_shape=[
            jax.ShapeDtypeStruct((1, side, width), F32),
            jax.ShapeDtypeStruct((1, 1, hidden, hidden), F32),
            jax.ShapeDtypeStruct((1, width, hidden), BF16),
            jax.ShapeDtypeStruct((rows, side), F32),
            jax.ShapeDtypeStruct((2, rows, side), BF16),
            jax.ShapeDtypeStruct((rows, hidden), BF16),
            jax.ShapeDtypeStruct((8, 128), F32),
        ],
        in_specs=[SMEM, SMEM] + [VMEM] * 6 + [ANY],
        out_specs=[ANY, VMEM, ANY, VMEM, VMEM, VMEM, VMEM],
        scratch_shapes=[
            pltpu.VMEM((rows, hidden), BF16),
            pltpu.VMEM((2, side, side), BF16),
            pltpu.VMEM((2, half, half), BF16),
            pltpu.VMEM((2, step, width), F32),
            pltpu.VMEM((side, hidden), BF16),
            pltpu.SemaphoreType.DMA((2,)),
            pltpu.SemaphoreType.DMA((2,)),
            pltpu.SemaphoreType.DMA((side // 256,)),
        ],
        compiler_params=pltpu.CompilerParams(vmem_limit_bytes=48 * 2**20),
        cost_estimate=pl.CostEstimate(
            flops=2 * rows * width * side * 3, bytes_accessed=20 * 2**20, transcendentals=0
        ),
    )(rep, owner, *groups, tri, g_inverse, a_inverse)


def last_kernel(rep_ref, square_ref, part_ref, x_ref, v_ref, inv_ref, u_in, u_out, ubuf, u_sem):
    oth = 1 - rep_ref[0]
    half = square_ref.shape[0]
    side = 2 * half
    inv = inv_ref[:1, :1]
    tile = 256
    stores = []
    for c in range(side // tile):
        cols = slice(c * tile, (c + 1) * tile)
        h, inner = divmod(c * tile, half)
        if h == 0:
            extra = dot_nt(x_ref[oth, :, half:], square_ref[inner : inner + tile, :])
        else:
            extra = dot(x_ref[oth, :, :half], square_ref[:, inner : inner + tile])
        mixed = (part_ref[:, cols] + extra).astype(BF16)
        ubuf[cols, :] = (dot_tn(mixed, v_ref[...]) * inv).astype(BF16)
        store = pltpu.make_async_copy(
            ubuf.at[pl.ds(c * tile, tile)], u_out.at[0, pl.ds(oth * side + c * tile, tile), :], u_sem.at[c]
        )
        store.start()
        stores.append(store)
    for store in stores:
        store.wait()


def finish(rep, square, part, xs, v, inv, u):
    side, hidden = part.shape[1], v.shape[1]
    return pl.pallas_call(
        last_kernel,
        name="finish",
        out_shape=jax.ShapeDtypeStruct(u.shape, BF16),
        in_specs=[SMEM] + [VMEM] * 5 + [ANY],
        out_specs=ANY,
        input_output_aliases={6: 0},
        scratch_shapes=[
            pltpu.VMEM((side, hidden), BF16),
            pltpu.SemaphoreType.DMA((side // 256,)),
        ],
        compiler_params=pltpu.CompilerParams(vmem_limit_bytes=24 * 2**20),
        cost_estimate=pl.CostEstimate(
            flops=2 * part.shape[0] * side * (side + hidden), bytes_accessed=4 * 2**20, transcendentals=0
        ),
    )(rep, square, part, xs, v, inv, u)


def local(tokens, cotangents, routes, owner, a_inverse, g_inverse):
    experts = lax.axis_size("expert")
    me = lax.axis_index("expert").astype(jnp.int32).reshape(1)
    rep = lax.axis_index("replica").astype(jnp.int32).reshape(1)
    swap = [(0, 1), (1, 0)]
    tri, square = fold(rep, a_inverse)
    tri = lax.ppermute(tri, "replica", swap)
    blocks = pack(me, routes, tokens, cotangents, experts)
    got = [None] * experts
    got[0] = blocks[0]
    for k in list(range(experts // 2, experts)) + list(range(1, experts // 2)):
        got[k] = lax.ppermute(blocks[k], "expert", [(i, i ^ k) for i in range(experts)])
    near = jnp.concatenate(got[: experts // 2], axis=0)
    far = jnp.concatenate(got[experts // 2 :], axis=0)
    near2 = lax.ppermute(near, "replica", swap)
    far2 = lax.ppermute(far, "replica", swap)
    square, far = lax.optimization_barrier((square, far))
    square = lax.ppermute(square, "replica", swap)
    a_factor, kept, u, part, xs, v, inv = products(
        rep, owner, [near, far, near2, far2], tri, g_inverse, a_inverse
    )
    return a_factor, kept, finish(rep, square, part, xs, v, inv, u)


def slot_table(route_block, expert_count, capacity):
    top_k = route_block.shape[1]
    route_ids = route_block.reshape(-1)
    in_window = route_ids < expert_count
    columns = lax.broadcasted_iota(jnp.int32, (route_ids.shape[0], expert_count), 1)
    one_hot = ((route_ids[:, None] == columns) & in_window[:, None]).astype(jnp.int32)
    before = jnp.cumsum(one_hot, axis=0) - one_hot
    position = jnp.sum(before * one_hot, axis=1)
    sentinel = expert_count * capacity
    slot_ids = jnp.where(in_window, route_ids * capacity + position, sentinel)
    source_ids = jnp.arange(route_ids.shape[0], dtype=jnp.int32) // top_k
    slot_token = jnp.zeros((sentinel + 1,), jnp.int32).at[slot_ids].set(source_ids)
    filled = jnp.zeros((sentinel + 1,), jnp.int32).at[slot_ids].set(1)
    return (slot_token[:sentinel], filled[:sentinel])


def local_any(tokens, cotangents, routes, owner, a_inverse, g_inverse):
    expert_count = lax.axis_size("expert")
    replica_count = lax.axis_size("replica")
    width = tokens.shape[1]
    hidden_width = cotangents.shape[1]
    slot_token, filled = slot_table(routes, expert_count, CAP)
    slot_mask = filled.astype(jnp.bfloat16)[:, None]
    send_x = (jnp.take(tokens, slot_token, axis=0) * slot_mask).reshape(expert_count, CAP, width)
    send_y = (jnp.take(cotangents, slot_token, axis=0) * slot_mask).reshape(
        expert_count, CAP, hidden_width
    )
    sent_counts = jnp.sum(filled.reshape(expert_count, CAP), axis=1).astype(jnp.bfloat16)
    recv_x, recv_y, recv_counts = (
        lax.all_to_all(send_x, "expert", split_axis=0, concat_axis=0, tiled=True),
        lax.all_to_all(send_y, "expert", split_axis=0, concat_axis=0, tiled=True),
        lax.all_to_all(sent_counts, "expert", split_axis=0, concat_axis=0, tiled=True),
    )
    rows_x = recv_x.reshape(-1, width)
    rows_y = recv_y.reshape(-1, hidden_width)
    block_rows = width // replica_count
    own_start = lax.axis_index("replica") * block_rows
    piece_x = lax.all_gather(rows_x, "replica", axis=0, tiled=True)
    piece_y = lax.all_gather(rows_y, "replica", axis=0, tiled=True)
    piece_counts = lax.all_gather(recv_counts, "replica", axis=0, tiled=True)
    columns = lax.dynamic_slice_in_dim(piece_x, own_start, block_rows, 1)
    a_next = jnp.dot(columns.T, piece_x, preferred_element_type=jnp.float32)
    g_next = jnp.dot(piece_y.T, piece_y, preferred_element_type=jnp.float32)
    count_next = jnp.sum(piece_counts.astype(jnp.float32))
    mixed_own = jnp.dot(a_inverse[0], piece_x.T, preferred_element_type=jnp.float32).astype(BF16)
    mixed = lax.all_gather(mixed_own, "replica", axis=0, tiled=True)
    right = jnp.dot(piece_y, g_inverse[0], preferred_element_type=jnp.float32).astype(BF16)
    update = (jnp.dot(mixed, right, preferred_element_type=jnp.float32) / count_next).astype(BF16)
    a_factor = (a_next / count_next)[None]
    keeper = owner[0] == lax.axis_index("replica")
    kept = jnp.where(keeper, g_next / count_next, jnp.zeros_like(g_next))[None, None]
    return (a_factor, kept, update[None])


def solution(mesh):
    placed = (
        P(("expert", "replica"), None),
        P(("expert", "replica"), None),
        P(("expert", "replica"), None),
        P("expert"),
        P("expert", "replica", None),
        P("expert", None, None),
    )
    return jax.shard_map(
        local if mesh.shape["replica"] == 2 else local_any,
        mesh=mesh,
        in_specs=placed,
        out_specs=(
            P("expert", "replica", None),
            P("replica", "expert", None, None),
            P("expert", None, None),
        ),
        check_vma=False,
    )
```

```python
import functools

import jax
import jax.numpy as jnp
from jax import lax
from jax.experimental import pallas as pl
from jax.experimental.pallas import tpu as pltpu
from jax.sharding import PartitionSpec as P


CAP = 12
MAIN = 8
EMPTY = 1024.0

PAD = 16
TILE = 256
RING = 4
AHEAD = 256


F32 = jnp.float32
BF16 = jnp.bfloat16
VMEM = pl.BlockSpec(memory_space=pltpu.VMEM)
SMEM = pl.BlockSpec(memory_space=pltpu.SMEM)
ANY = pl.BlockSpec(memory_space=pl.ANY)


def dot(a, b):
    return jnp.dot(a, b, preferred_element_type=F32)


def dot_nt(a, b):
    return lax.dot_general(a, b, (((1,), (1,)), ((), ())), preferred_element_type=F32)


def dot_tn(a, b):
    return lax.dot_general(a, b, (((0,), (0,)), ((), ())), preferred_element_type=F32)


def target(me, block, experts):
    inner = experts // (2 * RING)
    place = (me // (2 * inner) + block // inner) % RING
    return (place * inner + (me // 2 % inner ^ block % inner)) * 2 + me % 2


def pack_kernel(me_ref, *refs):
    me = me_ref[0]
    sources, out_refs = (refs[0:3], refs[3:6]), refs[6:]
    top, toks = refs[0].shape
    width, hidden = refs[1].shape[1], refs[2].shape[1]
    half = (width + hidden) // 2
    base, split = width + hidden, width - half
    span = len(sources) * MAIN
    rows = len(out_refs) * span
    row = lax.broadcasted_iota(jnp.int32, (rows, toks), 0)
    ids = target(me, row // span, 2 * len(out_refs))
    sub = row % MAIN
    low = sub < MAIN // 2
    earlier = lax.broadcasted_iota(jnp.int32, (toks, toks), 0) < lax.broadcasted_iota(
        jnp.int32, (toks, toks), 1
    )
    earlier = jnp.where(earlier, 1.0, 0.0).astype(BF16)
    picks, lows, highs = [], [], []
    full, full_rest = 0.0, 0.0
    for n, (routes_ref, _, _) in enumerate(sources):
        mine = row // MAIN % len(sources) == n
        chosen = jnp.zeros((rows, toks), F32)
        for k in range(top):
            chosen += jnp.where((routes_ref[k : k + 1, :] == ids) & mine, 1.0, 0.0)
        slot = jnp.where(chosen > 0.0, dot(chosen.astype(BF16), earlier), -1.0).astype(jnp.int32)
        pick = jnp.where(slot == sub, 1.0, 0.0)
        rest = jnp.where(slot == jnp.where(low, MAIN + sub, MAIN // 2 + sub), 1.0, 0.0)
        full += jnp.sum(pick, axis=1, keepdims=True)
        full_rest += jnp.sum(rest, axis=1, keepdims=True)
        picks.append(pick.astype(BF16))
        lows.append(jnp.where(low, rest, 0.0).astype(BF16))
        highs.append(jnp.where(low, 0.0, rest).astype(BF16))
    lane0 = lax.broadcasted_iota(jnp.int32, (rows, 128), 1) == 0
    low_lanes = lax.broadcasted_iota(jnp.int32, (rows, 128), 0) % MAIN < MAIN // 2

    def put(at, value):
        for q, ref in enumerate(out_refs):
            ref[:, at : at + value.shape[1]] = value[q * span : (q + 1) * span].astype(BF16)

    def x(which, cols):
        return sum(dot(w, refs[cols]) for w, (_, refs, _) in zip(which, sources))

    def y(which):
        return sum(dot(w, ref[...]) for w, (_, _, ref) in zip(which, sources))

    first = x(picks, (slice(None), slice(0, 128)))
    put(0, jnp.where(lane0 & (full == 0.0), EMPTY, first))
    put(128, x(picks, (slice(None), slice(128, width))))
    put(width, y(picks))
    rem = x(lows, (slice(None), slice(0, split))) + x(highs, (slice(None), slice(half, width)))
    put(base, jnp.where(lane0 & low_lanes & (full_rest == 0.0), EMPTY, rem[:, :128]))
    put(base + 128, rem[:, 128:])
    put(base + split, x(lows, (slice(None), slice(split, half))) + y(highs))


def pack(me, mine, other, blocks):
    toks, width = mine[1].shape
    width = (width + mine[2].shape[1]) * CAP // MAIN
    return pl.pallas_call(
        pack_kernel,
        name="pack",
        out_shape=[jax.ShapeDtypeStruct((2 * MAIN, width), BF16)] * blocks,
        in_specs=[SMEM] + [VMEM] * 6,
        out_specs=[VMEM] * blocks,
        compiler_params=pltpu.CompilerParams(vmem_limit_bytes=12 * 2**20),
        cost_estimate=pl.CostEstimate(
            flops=8 * blocks * MAIN * toks * width, bytes_accessed=3 * 2**20, transcendentals=0
        ),
    )(me, *mine, *other)


def fold_kernel(rep_ref, p_ref, s_ref, *refs):
    out_ref = refs[-1]
    half = p_ref.shape[1]
    p, s = p_ref[0].astype(F32), s_ref[0].astype(F32)
    row = lax.broadcasted_iota(jnp.int32, (half, half), 0)
    col = lax.broadcasted_iota(jnp.int32, (half, half), 1)
    out_ref[:half, :] = jnp.where(col >= row, p, s).astype(BF16)
    diagonal = jnp.sum(jnp.where(row == col, s, 0.0), axis=0, keepdims=True)
    out_ref[half : half + PAD, :] = jnp.broadcast_to(diagonal, (PAD, half)).astype(BF16)
    if len(refs) > 1:
        out_ref[half + PAD :, :] = refs[0][0]


def fold(rep, a_inverse):
    half = a_inverse.shape[1] // 2
    rows = half + PAD + AHEAD
    extra = [pl.BlockSpec((1, AHEAD, half), lambda i, rep: (0, 0, 2 * rep[0] + 1))] if AHEAD else []
    return pl.pallas_call(
        fold_kernel,
        name="fold",
        out_shape=jax.ShapeDtypeStruct((rows, half), BF16),
        grid_spec=pltpu.PrefetchScalarGridSpec(
            num_scalar_prefetch=1,
            grid=(1,),
            in_specs=[
                pl.BlockSpec((1, half, half), lambda i, rep: (0, 0, 2 * rep[0])),
                pl.BlockSpec((1, half, half), lambda i, rep: (0, 1, 2 * rep[0] + 1)),
                *extra,
            ],
            out_specs=pl.BlockSpec((rows, half), lambda i, rep: (0, 0)),
        ),
        compiler_params=pltpu.CompilerParams(vmem_limit_bytes=12 * 2**20),
        cost_estimate=pl.CostEstimate(flops=half * half, bytes_accessed=6 * half * half, transcendentals=0),
    )(rep, *[a_inverse] * (2 + len(extra)))


def square_kernel(rep_ref, q_ref, out_ref):
    out_ref[...] = q_ref[0, AHEAD:, :]


def square_of(rep, a_inverse):
    half = a_inverse.shape[1] // 2
    return pl.pallas_call(
        square_kernel,
        name="square",
        out_shape=jax.ShapeDtypeStruct((half - AHEAD, half), BF16),
        grid_spec=pltpu.PrefetchScalarGridSpec(
            num_scalar_prefetch=1,
            grid=(1,),
            in_specs=[pl.BlockSpec((1, half, half), lambda i, rep: (0, 0, 2 * rep[0] + 1))],
            out_specs=pl.BlockSpec((half - AHEAD, half), lambda i, rep: (0, 0)),
        ),
        compiler_params=pltpu.CompilerParams(vmem_limit_bytes=6 * 2**20),
        cost_estimate=pl.CostEstimate(flops=half * half, bytes_accessed=2 * half * half, transcendentals=0),
    )(rep, a_inverse)


def gather_rows(groups, x_ref, y_ref, at):
    cols = x_ref.shape[2]
    width = 2 * cols
    hidden = y_ref.shape[1]
    half = (width + hidden) // 2
    base = width + hidden
    start = at
    for ref in groups:
        count = ref.shape[0]
        x_ref[0, at : at + count, :] = ref[:, :cols]
        x_ref[1, at : at + count, :] = ref[:, cols:width]
        y_ref[at : at + count, :] = ref[:, width:base]
        at += count
    for ref in groups:
        count = ref.shape[0] // 2
        low = lax.broadcasted_iota(jnp.int32, (count, half), 0) % MAIN < MAIN // 2
        one, two = ref[:count, base:].astype(F32), ref[count:, base:].astype(F32)
        lo = jnp.where(low, one, pltpu.roll(two, MAIN // 2, 0)).astype(BF16)
        hi = jnp.where(low, pltpu.roll(one, count - MAIN // 2, 0), two).astype(BF16)
        x_ref[0, at : at + count, :] = lo[:, :cols]
        x_ref[1, at : at + count, : half - cols] = lo[:, cols:]
        x_ref[1, at : at + count, half - cols :] = hi[:, : width - half]
        y_ref[at : at + count, :] = hi[:, width - half :]
        at += count
    edge = x_ref[0, start:at, :128].astype(F32)
    empty = (lax.broadcasted_iota(jnp.int32, edge.shape, 1) == 0) & (edge == EMPTY)
    x_ref[0, start:at, :128] = jnp.where(empty, 0.0, edge).astype(BF16)
    return (at - start) - jnp.sum(jnp.where(empty, 1.0, 0.0))


def mix_rows(x_ref, rows, a_ref, ps_ref, rep, own_ref, part_ref):
    oth = 1 - rep
    side = x_ref.shape[2]
    half = side // 2
    own_at, oth_at = pl.multiple_of(rep * side, side), pl.multiple_of(oth * side, side)
    x_own, x_oth = x_ref[rep, rows, :], x_ref[oth, rows, :]
    for c in range(side // TILE):
        cols = slice(c * TILE, (c + 1) * TILE)
        own_ref[rows, cols] = (
            dot(x_own, a_ref[0, :, pl.ds(own_at + c * TILE, TILE)])
            + dot_nt(x_oth, a_ref[0, cols, pl.ds(oth_at, side)])
        ).astype(BF16)
    for c in range(side // TILE):
        h, inner = divmod(c * TILE, half)
        value = dot(x_own, a_ref[0, :, pl.ds(oth_at + c * TILE, TILE)]) + dot(
            x_oth[:, h * half : (h + 1) * half], ps_ref[h, :, inner : inner + TILE]
        )
        if h == 1 and AHEAD:
            value += dot(x_oth[:, :AHEAD], ps_ref[2, :AHEAD, inner : inner + TILE])
        if c * TILE < AHEAD:
            value += dot_nt(x_oth[:, half:], ps_ref[2, inner : inner + TILE, :])
            own_ref[rows, side + c * TILE : side + (c + 1) * TILE] = value.astype(BF16)
        else:
            part_ref[rows, c * TILE - AHEAD : (c + 1) * TILE - AHEAD] = value


def early_kernel(rep_ref, *refs, groups, unfold):
    blocks = refs[:groups]
    tri_ref, g_ref, a_ref, x_ref, y_ref, own_ref, part_ref, v_ref, count_ref = refs[groups : groups + 9]
    ps_ref = refs[-1]
    rep = rep_ref[0]
    half = tri_ref.shape[1]
    if unfold:
        if AHEAD:
            ps_ref[2, :AHEAD, :] = tri_ref[half + PAD :, :]
        mix = tri_ref[:half, :].astype(F32)
        mix_t = mix.T
        row = lax.broadcasted_iota(jnp.int32, (half, half), 0)
        col = lax.broadcasted_iota(jnp.int32, (half, half), 1)
        diagonal = tri_ref[half : half + 1, :].astype(F32)
        ps_ref[0] = jnp.where(col >= row, mix, mix_t).astype(BF16)
        ps_ref[1] = jnp.where(col < row, mix, jnp.where(col == row, diagonal, mix_t)).astype(BF16)
    else:
        ps_ref = tri_ref
    count = gather_rows(blocks, x_ref, y_ref, 0)
    count_ref[...] = jnp.full(count_ref.shape, count, F32)
    v_ref[...] = dot(y_ref[...], g_ref[0]).astype(BF16)
    mix_rows(x_ref, slice(0, x_ref.shape[1]), a_ref, ps_ref, rep, own_ref, part_ref)


def early(rep, groups, tri, g_inverse, a_inverse, unfold):
    rows = sum(g.shape[0] for g in groups) * CAP // MAIN
    _, side, width = a_inverse.shape
    hidden = g_inverse.shape[1]
    half = side // 2
    tri_shape = [jax.ShapeDtypeStruct((3 if AHEAD else 2, half, half), BF16)] if unfold else []
    return pl.pallas_call(
        functools.partial(early_kernel, groups=len(groups), unfold=unfold),
        name="early",
        out_shape=[
            jax.ShapeDtypeStruct((2, rows, side), BF16),
            jax.ShapeDtypeStruct((rows, hidden), BF16),
            jax.ShapeDtypeStruct((rows, side + AHEAD), BF16),
            jax.ShapeDtypeStruct((rows, side - AHEAD), F32),
            jax.ShapeDtypeStruct((rows, hidden), BF16),
            jax.ShapeDtypeStruct((8, 128), F32),
        ]
        + tri_shape,
        in_specs=[SMEM] + [VMEM] * (len(groups) + 3),
        out_specs=[VMEM] * (6 + unfold),
        compiler_params=pltpu.CompilerParams(vmem_limit_bytes=20 * 2**20),
        cost_estimate=pl.CostEstimate(flops=4 * rows * width * side, bytes_accessed=2**23, transcendentals=0),
    )(rep, *groups, tri, g_inverse, a_inverse)


def main_kernel(rep_ref, owner_ref, *refs, bundles):
    done = [refs[6 * n : 6 * (n + 1)] for n in range(bundles)]
    (
        a_out, kept_out, u_out, part_ref, xo_ref, v_ref, inv_ref,
        x_ref, y_ref, own_ref, abuf, gbuf, ubuf, a_sem, g_sem, u_sem,
    ) = refs[6 * bundles :]
    rep = rep_ref[0]
    oth = 1 - rep
    side = x_ref.shape[2]
    at = 0
    count = 0.0
    for x_in, y_in, own_in, part_in, v_in, count_in in done:
        more = at + y_in.shape[0]
        x_ref[:, at:more, :] = x_in[...]
        y_ref[at:more, :] = y_in[...]
        own_ref[at:more, :] = own_in[...]
        part_ref[at:more, :] = part_in[...]
        v_ref[at:more, :] = v_in[...]
        count = count + count_in[...]
        at = more
    inv = 1.0 / count
    inv_ref[...] = inv
    inv = inv[:1, :1]

    writes = []
    for i in range(side // TILE):
        lhs = x_ref[rep, :, i * TILE : (i + 1) * TILE]
        for h in range(2):
            abuf[i, :, h * side : (h + 1) * side] = dot_tn(lhs, x_ref[h]) * inv
        write = pltpu.make_async_copy(abuf.at[i], a_out.at[0, pl.ds(i * TILE, TILE), :], a_sem.at[i])
        write.start()
        writes.append(write)

    keep = jnp.where(owner_ref[0] == rep, 1.0, 0.0) * inv
    gbuf[...] = dot_tn(y_ref[...], y_ref[...]) * keep
    write = pltpu.make_async_copy(gbuf, kept_out.at[0, 0], g_sem)
    write.start()
    writes.append(write)

    xo_ref[...] = x_ref[oth, :, AHEAD:]
    for c in range((side + AHEAD) // TILE):
        cols = slice(c * TILE, (c + 1) * TILE)
        ubuf[cols, :] = (dot_tn(own_ref[:, cols], v_ref[...]) * inv).astype(BF16)
        to = rep * side + c * TILE if c * TILE < side else oth * side + c * TILE - side
        write = pltpu.make_async_copy(
            ubuf.at[pl.ds(c * TILE, TILE)], u_out.at[0, pl.ds(to, TILE), :], u_sem.at[c]
        )
        write.start()
        writes.append(write)
    for write in writes:
        write.wait()


def products(rep, owner, done, a_shape, hidden):
    rows = sum(d[1].shape[0] for d in done)
    _, side, width = a_shape
    return pl.pallas_call(
        functools.partial(main_kernel, bundles=len(done)),
        name="products",
        out_shape=[
            jax.ShapeDtypeStruct((1, side, width), F32),
            jax.ShapeDtypeStruct((1, 1, hidden, hidden), F32),
            jax.ShapeDtypeStruct((1, width, hidden), BF16),
            jax.ShapeDtypeStruct((rows, side - AHEAD), F32),
            jax.ShapeDtypeStruct((rows, side - AHEAD), BF16),
            jax.ShapeDtypeStruct((rows, hidden), BF16),
            jax.ShapeDtypeStruct((8, 128), F32),
        ],
        in_specs=[SMEM, SMEM] + [VMEM] * (6 * len(done)),
        out_specs=[ANY, ANY, ANY, VMEM, VMEM, VMEM, VMEM],
        scratch_shapes=[
            pltpu.VMEM((2, rows, side), BF16),
            pltpu.VMEM((rows, hidden), BF16),
            pltpu.VMEM((rows, side + AHEAD), BF16),
            pltpu.VMEM((side // TILE, TILE, width), F32),
            pltpu.VMEM((hidden, hidden), F32),
            pltpu.VMEM((side + AHEAD, hidden), BF16),
            pltpu.SemaphoreType.DMA((side // TILE,)),
            pltpu.SemaphoreType.DMA,
            pltpu.SemaphoreType.DMA(((side + AHEAD) // TILE,)),
        ],
        compiler_params=pltpu.CompilerParams(vmem_limit_bytes=36 * 2**20),
        cost_estimate=pl.CostEstimate(
            flops=4 * rows * width * side, bytes_accessed=12 * 2**20, transcendentals=0
        ),
    )(rep, owner, *[value for d in done for value in d])


def last_kernel(rep_ref, square_ref, part_ref, x_ref, v_ref, inv_ref, u_in, u_out, ubuf, u_sem):
    oth = 1 - rep_ref[0]
    rest, half = square_ref.shape
    side = 2 * half
    inv = inv_ref[:1, :1]
    stores = []
    for c in range((half + rest) // TILE):
        cols = slice(c * TILE, (c + 1) * TILE)
        at = c * TILE - rest
        if at < 0:
            extra = dot_nt(x_ref[:, rest:], square_ref[cols, :])
        else:
            extra = dot(x_ref[:, :rest], square_ref[:, at : at + TILE])
        mixed = (part_ref[:, cols] + extra).astype(BF16)
        ubuf[cols, :] = (dot_tn(mixed, v_ref[...]) * inv).astype(BF16)
        store = pltpu.make_async_copy(
            ubuf.at[pl.ds(c * TILE, TILE)],
            u_out.at[0, pl.ds(oth * side + half - rest + c * TILE, TILE), :],
            u_sem.at[c],
        )
        store.start()
        stores.append(store)
    for store in stores:
        store.wait()


def finish(rep, square, part, x, v, inv, u):
    side, hidden = part.shape[1], v.shape[1]
    return pl.pallas_call(
        last_kernel,
        name="finish",
        out_shape=jax.ShapeDtypeStruct(u.shape, BF16),
        in_specs=[SMEM] + [VMEM] * 5 + [ANY],
        out_specs=ANY,
        input_output_aliases={6: 0},
        scratch_shapes=[
            pltpu.VMEM((side, hidden), BF16),
            pltpu.SemaphoreType.DMA((side // TILE,)),
        ],
        compiler_params=pltpu.CompilerParams(vmem_limit_bytes=16 * 2**20),
        cost_estimate=pl.CostEstimate(
            flops=2 * part.shape[0] * side * (side + hidden), bytes_accessed=4 * 2**20, transcendentals=0
        ),
    )(rep, square, part, x, v, inv, u)


def parts(experts):
    inner = experts // (2 * RING)
    half = inner // 2
    return [
        list(range(inner)),
        [s * inner + w for s in (1, 3) for w in range(half)],
        [s * inner + w for s in (1, 3) for w in range(half, inner)],
        list(range(2 * inner, 3 * inner)),
    ]


def local(tokens, cotangents, routes, owner, a_inverse, g_inverse):
    experts = lax.axis_size("expert")
    me = lax.axis_index("expert").astype(jnp.int32).reshape(1)
    rep = lax.axis_index("replica").astype(jnp.int32).reshape(1)

    def swap(value):
        return lax.ppermute(value, "replica", [(0, 1), (1, 0)])

    def trade(value, to):
        return lax.ppermute(value, "expert", [(i, to(i)) for i in range(experts)])

    tri = swap(fold(rep, a_inverse))
    mine = (routes.T, tokens, cotangents)
    other = tuple(trade(value, lambda i: i ^ 1) for value in mine)
    blocks = pack(me, mine, other, experts // 2)
    got = [blocks[0]]
    for q in range(1, experts // 2):
        got.append(trade(blocks[q], lambda i, q=q: target(i, q, experts)))
    groups = [jnp.concatenate([got[q] for q in part], axis=0) for part in parts(experts)]
    others = [swap(group) for group in groups]
    square = square_of(rep, a_inverse)
    square = swap(square)
    *first, ps = early(rep, groups, tri, g_inverse, a_inverse, True)
    second = early(rep, others[:3], ps, g_inverse, a_inverse, False)
    third = early(rep, others[3:], ps, g_inverse, a_inverse, False)
    a_factor, kept, u, part, xo, v, inv = products(
        rep, owner, (first, second, third), a_inverse.shape, g_inverse.shape[1]
    )
    return a_factor, kept, finish(rep, square, part, xo, v, inv, u)


def slot_table(route_block, expert_count, capacity):
    top_k = route_block.shape[1]
    route_ids = route_block.reshape(-1)
    in_window = route_ids < expert_count
    columns = lax.broadcasted_iota(jnp.int32, (route_ids.shape[0], expert_count), 1)
    one_hot = ((route_ids[:, None] == columns) & in_window[:, None]).astype(jnp.int32)
    before = jnp.cumsum(one_hot, axis=0) - one_hot
    position = jnp.sum(before * one_hot, axis=1)
    sentinel = expert_count * capacity
    slot_ids = jnp.where(in_window, route_ids * capacity + position, sentinel)
    source_ids = jnp.arange(route_ids.shape[0], dtype=jnp.int32) // top_k
    slot_token = jnp.zeros((sentinel + 1,), jnp.int32).at[slot_ids].set(source_ids)
    filled = jnp.zeros((sentinel + 1,), jnp.int32).at[slot_ids].set(1)
    return (slot_token[:sentinel], filled[:sentinel])


def local_any(tokens, cotangents, routes, owner, a_inverse, g_inverse):
    expert_count = lax.axis_size("expert")
    replica_count = lax.axis_size("replica")
    width = tokens.shape[1]
    hidden_width = cotangents.shape[1]
    slot_token, filled = slot_table(routes, expert_count, CAP)
    slot_mask = filled.astype(jnp.bfloat16)[:, None]
    send_x = (jnp.take(tokens, slot_token, axis=0) * slot_mask).reshape(expert_count, CAP, width)
    send_y = (jnp.take(cotangents, slot_token, axis=0) * slot_mask).reshape(
        expert_count, CAP, hidden_width
    )
    sent_counts = jnp.sum(filled.reshape(expert_count, CAP), axis=1).astype(jnp.bfloat16)
    recv_x, recv_y, recv_counts = (
        lax.all_to_all(send_x, "expert", split_axis=0, concat_axis=0, tiled=True),
        lax.all_to_all(send_y, "expert", split_axis=0, concat_axis=0, tiled=True),
        lax.all_to_all(sent_counts, "expert", split_axis=0, concat_axis=0, tiled=True),
    )
    rows_x = recv_x.reshape(-1, width)
    rows_y = recv_y.reshape(-1, hidden_width)
    block_rows = width // replica_count
    own_start = lax.axis_index("replica") * block_rows
    piece_x = lax.all_gather(rows_x, "replica", axis=0, tiled=True)
    piece_y = lax.all_gather(rows_y, "replica", axis=0, tiled=True)
    piece_counts = lax.all_gather(recv_counts, "replica", axis=0, tiled=True)
    columns = lax.dynamic_slice_in_dim(piece_x, own_start, block_rows, 1)
    a_next = jnp.dot(columns.T, piece_x, preferred_element_type=jnp.float32)
    g_next = jnp.dot(piece_y.T, piece_y, preferred_element_type=jnp.float32)
    count_next = jnp.sum(piece_counts.astype(jnp.float32))
    mixed_own = jnp.dot(a_inverse[0], piece_x.T, preferred_element_type=jnp.float32).astype(BF16)
    mixed = lax.all_gather(mixed_own, "replica", axis=0, tiled=True)
    right = jnp.dot(piece_y, g_inverse[0], preferred_element_type=jnp.float32).astype(BF16)
    update = (jnp.dot(mixed, right, preferred_element_type=jnp.float32) / count_next).astype(BF16)
    a_factor = (a_next / count_next)[None]
    keeper = owner[0] == lax.axis_index("replica")
    kept = jnp.where(keeper, g_next / count_next, jnp.zeros_like(g_next))[None, None]
    return (a_factor, kept, update[None])


def solution(mesh):
    placed = (
        P(("expert", "replica"), None),
        P(("expert", "replica"), None),
        P(("expert", "replica"), None),
        P("expert"),
        P("expert", "replica", None),
        P("expert", None, None),
    )
    pair = mesh.shape["replica"] == 2
    return jax.shard_map(
        local if pair else local_any,
        mesh=mesh,
        in_specs=placed,
        out_specs=(
            P("expert", "replica", None),
            P("replica", "expert", None, None),
            P("expert", None, None),
        ),
        check_vma=False,
    )
```

```python
import functools

import jax
import jax.numpy as jnp
from jax import lax
from jax.experimental import pallas as pl
from jax.experimental.pallas import tpu as pltpu
from jax.sharding import PartitionSpec as P


CAP = 12
MAIN = 8
EMPTY = 1024.0

PAD = 8
TILE = 256
RING = 4
FOLD_VMEM = 50 * 2**20
AHEAD = 128


F32 = jnp.float32
BF16 = jnp.bfloat16
VMEM = pl.BlockSpec(memory_space=pltpu.VMEM)
SMEM = pl.BlockSpec(memory_space=pltpu.SMEM)
ANY = pl.BlockSpec(memory_space=pl.ANY)


def tiles(start, stop):
    return [(at, min(at + TILE, stop)) for at in range(start, stop, TILE)]


def dot(a, b):
    return jnp.dot(a, b, preferred_element_type=F32)


def dot_nt(a, b):
    return lax.dot_general(a, b, (((1,), (1,)), ((), ())), preferred_element_type=F32)


def dot_tn(a, b):
    return lax.dot_general(a, b, (((0,), (0,)), ((), ())), preferred_element_type=F32)


def target(me, block, experts):
    inner = experts // (2 * RING)
    place = (me // (2 * inner) + block // inner) % RING
    return (place * inner + (me // 2 % inner ^ block % inner)) * 2 + me % 2


def pack_kernel(me_ref, *refs):
    me = me_ref[0]
    sources, out_refs = (refs[0:3], refs[3:6]), refs[6:]
    top, toks = refs[0].shape
    width, hidden = refs[1].shape[1], refs[2].shape[1]
    half = (width + hidden) // 2
    base, split = width + hidden, width - half
    span = len(sources) * MAIN
    rows = len(out_refs) * span
    row = lax.broadcasted_iota(jnp.int32, (rows, toks), 0)
    ids = target(me, row // span, 2 * len(out_refs))
    sub = row % MAIN
    low = sub < MAIN // 2
    earlier = lax.broadcasted_iota(jnp.int32, (toks, toks), 0) < lax.broadcasted_iota(
        jnp.int32, (toks, toks), 1
    )
    earlier = jnp.where(earlier, 1.0, 0.0).astype(BF16)
    picks, lows, highs = [], [], []
    full, full_rest = 0.0, 0.0
    for n, (routes_ref, _, _) in enumerate(sources):
        mine = row // MAIN % len(sources) == n
        chosen = jnp.zeros((rows, toks), F32)
        for k in range(top):
            chosen += jnp.where((routes_ref[k : k + 1, :] == ids) & mine, 1.0, 0.0)
        slot = jnp.where(chosen > 0.0, dot(chosen.astype(BF16), earlier), -1.0).astype(jnp.int32)
        pick = jnp.where(slot == sub, 1.0, 0.0)
        rest = jnp.where(slot == jnp.where(low, MAIN + sub, MAIN // 2 + sub), 1.0, 0.0)
        full += jnp.sum(pick, axis=1, keepdims=True)
        full_rest += jnp.sum(rest, axis=1, keepdims=True)
        picks.append(pick.astype(BF16))
        lows.append(jnp.where(low, rest, 0.0).astype(BF16))
        highs.append(jnp.where(low, 0.0, rest).astype(BF16))
    lane0 = lax.broadcasted_iota(jnp.int32, (rows, 128), 1) == 0
    low_lanes = lax.broadcasted_iota(jnp.int32, (rows, 128), 0) % MAIN < MAIN // 2

    def put(at, value):
        for q, ref in enumerate(out_refs):
            ref[:, at : at + value.shape[1]] = value[q * span : (q + 1) * span].astype(BF16)

    def x(which, cols):
        return sum(dot(w, refs[cols]) for w, (_, refs, _) in zip(which, sources))

    def y(which):
        return sum(dot(w, ref[...]) for w, (_, _, ref) in zip(which, sources))

    first = x(picks, (slice(None), slice(0, 128)))
    put(0, jnp.where(lane0 & (full == 0.0), EMPTY, first))
    put(128, x(picks, (slice(None), slice(128, width))))
    put(width, y(picks))
    rem = x(lows, (slice(None), slice(0, split))) + x(highs, (slice(None), slice(half, width)))
    put(base, jnp.where(lane0 & low_lanes & (full_rest == 0.0), EMPTY, rem[:, :128]))
    put(base + 128, rem[:, 128:])
    put(base + split, x(lows, (slice(None), slice(split, half))) + y(highs))


def pack(me, mine, other, blocks):
    toks, width = mine[1].shape
    width = (width + mine[2].shape[1]) * CAP // MAIN
    return pl.pallas_call(
        pack_kernel,
        name="pack",
        out_shape=[jax.ShapeDtypeStruct((2 * MAIN, width), BF16)] * blocks,
        in_specs=[SMEM] + [VMEM] * 6,
        out_specs=[VMEM] * blocks,
        compiler_params=pltpu.CompilerParams(vmem_limit_bytes=12 * 2**20),
        cost_estimate=pl.CostEstimate(
            flops=8 * blocks * MAIN * toks * width, bytes_accessed=3 * 2**20, transcendentals=0
        ),
    )(me, *mine, *other)


def fold_kernel(rep_ref, a_hbm, out_ref, p_ref, s_ref, sems):
    half = p_ref.shape[0]
    at = pl.multiple_of(rep_ref[0] * 2 * half, 2 * half)
    step = half // 4
    loads = []
    for top in range(0, half, step):
        for ref, down, over in ((p_ref, 0, 0), (s_ref, half, half)):
            src = a_hbm.at[0, pl.ds(down + top, step), pl.ds(at + over, half)]
            loads.append(pltpu.make_async_copy(src, ref.at[pl.ds(top, step)], sems.at[len(loads)]))
    if AHEAD:
        src = a_hbm.at[0, pl.ds(0, AHEAD), pl.ds(at + half, half)]
        loads.append(pltpu.make_async_copy(src, out_ref.at[pl.ds(half + PAD, AHEAD)], sems.at[len(loads)]))
    for load in loads:
        load.start()
    row = lax.broadcasted_iota(jnp.int32, (half, half), 0)
    col = lax.broadcasted_iota(jnp.int32, (half, half), 1)
    for load in loads:
        load.wait()
    p, s = p_ref[...].astype(F32), s_ref[...].astype(F32)
    out_ref[:half, :] = jnp.where(col >= row, p, s).astype(BF16)
    diagonal = jnp.sum(jnp.where(row == col, s, 0.0), axis=0, keepdims=True)
    out_ref[half : half + PAD, :] = jnp.broadcast_to(diagonal, (PAD, half)).astype(BF16)


def fold(rep, a_inverse):
    half = a_inverse.shape[1] // 2
    rows = half + PAD + AHEAD
    return pl.pallas_call(
        fold_kernel,
        name="fold",
        out_shape=jax.ShapeDtypeStruct((rows, half), BF16),
        in_specs=[SMEM, ANY],
        out_specs=VMEM,
        scratch_shapes=[
            pltpu.VMEM((half, half), BF16),
            pltpu.VMEM((half, half), BF16),
            pltpu.SemaphoreType.DMA((9,)),
        ],
        compiler_params=pltpu.CompilerParams(vmem_limit_bytes=FOLD_VMEM),
        cost_estimate=pl.CostEstimate(flops=half * half, bytes_accessed=6 * half * half, transcendentals=0),
    )(rep, a_inverse)


def square_kernel(rep_ref, q_ref, out_ref):
    out_ref[...] = q_ref[0, AHEAD:, :]


def square_of(rep, a_inverse):
    half = a_inverse.shape[1] // 2
    return pl.pallas_call(
        square_kernel,
        name="square",
        out_shape=jax.ShapeDtypeStruct((half - AHEAD, half), BF16),
        grid_spec=pltpu.PrefetchScalarGridSpec(
            num_scalar_prefetch=1,
            grid=(1,),
            in_specs=[pl.BlockSpec((1, half, half), lambda i, rep: (0, 0, 2 * rep[0] + 1))],
            out_specs=pl.BlockSpec((half - AHEAD, half), lambda i, rep: (0, 0)),
        ),
        compiler_params=pltpu.CompilerParams(vmem_limit_bytes=6 * 2**20),
        cost_estimate=pl.CostEstimate(flops=half * half, bytes_accessed=2 * half * half, transcendentals=0),
    )(rep, a_inverse)


def gather_rows(groups, x_ref, y_ref, at):
    cols = x_ref.shape[2]
    width = 2 * cols
    hidden = y_ref.shape[1]
    half = (width + hidden) // 2
    base = width + hidden
    start = at
    for ref in groups:
        count = ref.shape[0]
        x_ref[0, at : at + count, :] = ref[:, :cols]
        x_ref[1, at : at + count, :] = ref[:, cols:width]
        y_ref[at : at + count, :] = ref[:, width:base]
        at += count
    for ref in groups:
        count = ref.shape[0] // 2
        low = lax.broadcasted_iota(jnp.int32, (count, half), 0) % MAIN < MAIN // 2
        one, two = ref[:count, base:].astype(F32), ref[count:, base:].astype(F32)
        lo = jnp.where(low, one, pltpu.roll(two, MAIN // 2, 0)).astype(BF16)
        hi = jnp.where(low, pltpu.roll(one, count - MAIN // 2, 0), two).astype(BF16)
        x_ref[0, at : at + count, :] = lo[:, :cols]
        x_ref[1, at : at + count, : half - cols] = lo[:, cols:]
        x_ref[1, at : at + count, half - cols :] = hi[:, : width - half]
        y_ref[at : at + count, :] = hi[:, width - half :]
        at += count
    edge = x_ref[0, start:at, :128].astype(F32)
    empty = (lax.broadcasted_iota(jnp.int32, edge.shape, 1) == 0) & (edge == EMPTY)
    x_ref[0, start:at, :128] = jnp.where(empty, 0.0, edge).astype(BF16)
    return (at - start) - jnp.sum(jnp.where(empty, 1.0, 0.0))


def mix_rows(x_ref, rows, a_ref, ps_ref, rep, own_ref, part_ref):
    oth = 1 - rep
    side = x_ref.shape[2]
    half = side // 2
    own_at, oth_at = pl.multiple_of(rep * side, side), pl.multiple_of(oth * side, side)
    x_own, x_oth = x_ref[rep, rows, :], x_ref[oth, rows, :]
    for c in range(side // TILE):
        cols = slice(c * TILE, (c + 1) * TILE)
        own_ref[rows, cols] = (
            dot(x_own, a_ref[0, :, pl.ds(own_at + c * TILE, TILE)])
            + dot_nt(x_oth, a_ref[0, cols, pl.ds(oth_at, side)])
        ).astype(BF16)
    for c in range(side // TILE):
        h, inner = divmod(c * TILE, half)
        value = dot(x_own, a_ref[0, :, pl.ds(oth_at + c * TILE, TILE)]) + dot(
            x_oth[:, h * half : (h + 1) * half], ps_ref[h, :, inner : inner + TILE]
        )
        if h == 1 and AHEAD:
            value += dot(x_oth[:, :AHEAD], ps_ref[2, :AHEAD, inner : inner + TILE])
        ready = min(max(AHEAD - c * TILE, 0), TILE)
        if ready:
            full = value[:, :ready] + dot_nt(x_oth[:, half:], ps_ref[2, inner : inner + ready, :])
            own_ref[rows, side + c * TILE : side + c * TILE + ready] = full.astype(BF16)
        if ready < TILE:
            part_ref[rows, c * TILE + ready - AHEAD : (c + 1) * TILE - AHEAD] = value[:, ready:]


def early_kernel(rep_ref, *refs, groups, unfold):
    blocks = refs[:groups]
    tri_ref, g_ref, a_ref, x_ref, y_ref, own_ref, part_ref, v_ref, count_ref = refs[groups : groups + 9]
    ps_ref = refs[-1]
    rep = rep_ref[0]
    half = tri_ref.shape[1]
    if unfold:
        if AHEAD:
            ps_ref[2, :AHEAD, :] = tri_ref[half + PAD :, :]
        mix = tri_ref[:half, :].astype(F32)
        mix_t = mix.T
        row = lax.broadcasted_iota(jnp.int32, (half, half), 0)
        col = lax.broadcasted_iota(jnp.int32, (half, half), 1)
        diagonal = tri_ref[half : half + 1, :].astype(F32)
        ps_ref[0] = jnp.where(col >= row, mix, mix_t).astype(BF16)
        ps_ref[1] = jnp.where(col < row, mix, jnp.where(col == row, diagonal, mix_t)).astype(BF16)
    else:
        ps_ref = tri_ref
    count = gather_rows(blocks, x_ref, y_ref, 0)
    count_ref[...] = jnp.full(count_ref.shape, count, F32)
    v_ref[...] = dot(y_ref[...], g_ref[0]).astype(BF16)
    mix_rows(x_ref, slice(0, x_ref.shape[1]), a_ref, ps_ref, rep, own_ref, part_ref)


def early(rep, groups, tri, g_inverse, a_inverse, unfold):
    rows = sum(g.shape[0] for g in groups) * CAP // MAIN
    _, side, width = a_inverse.shape
    hidden = g_inverse.shape[1]
    half = side // 2
    tri_shape = [jax.ShapeDtypeStruct((3 if AHEAD else 2, half, half), BF16)] if unfold else []
    return pl.pallas_call(
        functools.partial(early_kernel, groups=len(groups), unfold=unfold),
        name="early",
        out_shape=[
            jax.ShapeDtypeStruct((2, rows, side), BF16),
            jax.ShapeDtypeStruct((rows, hidden), BF16),
            jax.ShapeDtypeStruct((rows, side + AHEAD), BF16),
            jax.ShapeDtypeStruct((rows, side - AHEAD), F32),
            jax.ShapeDtypeStruct((rows, hidden), BF16),
            jax.ShapeDtypeStruct((8, 128), F32),
        ]
        + tri_shape,
        in_specs=[SMEM] + [VMEM] * (len(groups) + 3),
        out_specs=[VMEM] * (6 + unfold),
        compiler_params=pltpu.CompilerParams(vmem_limit_bytes=20 * 2**20),
        cost_estimate=pl.CostEstimate(flops=4 * rows * width * side, bytes_accessed=2**23, transcendentals=0),
    )(rep, *groups, tri, g_inverse, a_inverse)


def main_kernel(rep_ref, owner_ref, *refs, groups, bundles):
    blocks = refs[:groups]
    done = [refs[groups + 6 * n : groups + 6 * (n + 1)] for n in range(bundles)]
    (
        ps_ref, g_ref, a_ref,
        a_out, kept_out, u_out, part_ref, xo_ref, v_ref, inv_ref,
        x_ref, y_ref, own_ref, abuf, gbuf, ubuf, a_sem, g_sem, u_sem,
    ) = refs[groups + 6 * bundles :]
    rep = rep_ref[0]
    oth = 1 - rep
    side = x_ref.shape[2]
    at = 0
    count = 0.0
    for x_in, y_in, own_in, part_in, v_in, count_in in done:
        more = at + y_in.shape[0]
        x_ref[:, at:more, :] = x_in[...]
        y_ref[at:more, :] = y_in[...]
        own_ref[at:more, :] = own_in[...]
        part_ref[at:more, :] = part_in[...]
        v_ref[at:more, :] = v_in[...]
        count = count + count_in[...]
        at = more
    count = count + gather_rows(blocks, x_ref, y_ref, at)
    v_ref[at:, :] = dot(y_ref[at:, :], g_ref[0]).astype(BF16)
    mix_rows(x_ref, slice(at, x_ref.shape[1]), a_ref, ps_ref, rep, own_ref, part_ref)
    inv = 1.0 / count
    inv_ref[...] = inv
    inv = inv[:1, :1]

    writes = []
    for i in range(side // TILE):
        lhs = x_ref[rep, :, i * TILE : (i + 1) * TILE]
        for h in range(2):
            abuf[i, :, h * side : (h + 1) * side] = dot_tn(lhs, x_ref[h]) * inv
        write = pltpu.make_async_copy(abuf.at[i], a_out.at[0, pl.ds(i * TILE, TILE), :], a_sem.at[i])
        write.start()
        writes.append(write)

    keep = jnp.where(owner_ref[0] == rep, 1.0, 0.0) * inv
    gbuf[...] = dot_tn(y_ref[...], y_ref[...]) * keep
    write = pltpu.make_async_copy(gbuf, kept_out.at[0, 0], g_sem)
    write.start()
    writes.append(write)

    xo_ref[...] = x_ref[oth, :, AHEAD:]
    for n, (c0, c1) in enumerate(tiles(0, side) + tiles(side, side + AHEAD)):
        ubuf[c0:c1, :] = (dot_tn(own_ref[:, c0:c1], v_ref[...]) * inv).astype(BF16)
        to = rep * side + c0 if c0 < side else oth * side + c0 - side
        write = pltpu.make_async_copy(
            ubuf.at[pl.ds(c0, c1 - c0)], u_out.at[0, pl.ds(to, c1 - c0), :], u_sem.at[n]
        )
        write.start()
        writes.append(write)
    for write in writes:
        write.wait()


def products(rep, owner, groups, done, ps, g_inverse, a_inverse):
    rows = sum(d[1].shape[0] for d in done) + sum(g.shape[0] for g in groups) * CAP // MAIN
    _, side, width = a_inverse.shape
    hidden = g_inverse.shape[1]
    return pl.pallas_call(
        functools.partial(main_kernel, groups=len(groups), bundles=len(done)),
        name="products",
        out_shape=[
            jax.ShapeDtypeStruct((1, side, width), F32),
            jax.ShapeDtypeStruct((1, 1, hidden, hidden), F32),
            jax.ShapeDtypeStruct((1, width, hidden), BF16),
            jax.ShapeDtypeStruct((rows, side - AHEAD), F32),
            jax.ShapeDtypeStruct((rows, side - AHEAD), BF16),
            jax.ShapeDtypeStruct((rows, hidden), BF16),
            jax.ShapeDtypeStruct((8, 128), F32),
        ],
        in_specs=[SMEM, SMEM] + [VMEM] * (len(groups) + 6 * len(done) + 3),
        out_specs=[ANY, ANY, ANY, VMEM, VMEM, VMEM, VMEM],
        scratch_shapes=[
            pltpu.VMEM((2, rows, side), BF16),
            pltpu.VMEM((rows, hidden), BF16),
            pltpu.VMEM((rows, side + AHEAD), BF16),
            pltpu.VMEM((side // TILE, TILE, width), F32),
            pltpu.VMEM((hidden, hidden), F32),
            pltpu.VMEM((side + AHEAD, hidden), BF16),
            pltpu.SemaphoreType.DMA((side // TILE,)),
            pltpu.SemaphoreType.DMA,
            pltpu.SemaphoreType.DMA((len(tiles(0, side) + tiles(side, side + AHEAD)),)),
        ],
        compiler_params=pltpu.CompilerParams(vmem_limit_bytes=36 * 2**20),
        cost_estimate=pl.CostEstimate(
            flops=4 * rows * width * side, bytes_accessed=12 * 2**20, transcendentals=0
        ),
    )(rep, owner, *groups, *[value for d in done for value in d], ps, g_inverse, a_inverse)


def last_kernel(rep_ref, square_ref, part_ref, x_ref, v_ref, inv_ref, u_in, u_out, ubuf, u_sem):
    oth = 1 - rep_ref[0]
    rest, half = square_ref.shape
    side = 2 * half
    inv = inv_ref[:1, :1]
    stores = []
    for n, (c0, c1) in enumerate(tiles(rest, rest + half) + tiles(0, rest)):
        if c0 < rest:
            extra = dot_nt(x_ref[:, rest:], square_ref[c0:c1, :])
        else:
            extra = dot(x_ref[:, :rest], square_ref[:, c0 - rest : c1 - rest])
        mixed = (part_ref[:, c0:c1] + extra).astype(BF16)
        ubuf[c0:c1, :] = (dot_tn(mixed, v_ref[...]) * inv).astype(BF16)
        store = pltpu.make_async_copy(
            ubuf.at[pl.ds(c0, c1 - c0)],
            u_out.at[0, pl.ds(oth * side + half - rest + c0, c1 - c0), :],
            u_sem.at[n],
        )
        store.start()
        stores.append(store)
    for store in stores:
        store.wait()


def finish(rep, square, part, x, v, inv, u):
    side, hidden = part.shape[1], v.shape[1]
    return pl.pallas_call(
        last_kernel,
        name="finish",
        out_shape=jax.ShapeDtypeStruct(u.shape, BF16),
        in_specs=[SMEM] + [VMEM] * 5 + [ANY],
        out_specs=ANY,
        input_output_aliases={6: 0},
        scratch_shapes=[
            pltpu.VMEM((side, hidden), BF16),
            pltpu.SemaphoreType.DMA((side // TILE + 2,)),
        ],
        compiler_params=pltpu.CompilerParams(vmem_limit_bytes=16 * 2**20),
        cost_estimate=pl.CostEstimate(
            flops=2 * part.shape[0] * side * (side + hidden), bytes_accessed=4 * 2**20, transcendentals=0
        ),
    )(rep, square, part, x, v, inv, u)


def parts(experts):
    inner = experts // (2 * RING)
    half = inner // 2
    return [
        list(range(inner)),
        [s * inner + w for s in (1, 3) for w in range(half)],
        [s * inner + w for s in (1, 3) for w in range(half, inner)],
        list(range(2 * inner, 3 * inner)),
    ]


def local(tokens, cotangents, routes, owner, a_inverse, g_inverse):
    experts = lax.axis_size("expert")
    me = lax.axis_index("expert").astype(jnp.int32).reshape(1)
    rep = lax.axis_index("replica").astype(jnp.int32).reshape(1)

    def swap(value):
        return lax.ppermute(value, "replica", [(0, 1), (1, 0)])

    def trade(value, to):
        return lax.ppermute(value, "expert", [(i, to(i)) for i in range(experts)])

    tri = fold(rep, a_inverse)
    tri = swap(tri)
    mine = (routes.T, tokens, cotangents)
    other = tuple(trade(value, lambda i: i ^ 1) for value in mine)
    blocks = pack(me, mine, other, experts // 2)
    got = [blocks[0]]
    for q in range(1, experts // 2):
        got.append(trade(blocks[q], lambda i, q=q: target(i, q, experts)))
    groups = [jnp.concatenate([got[q] for q in part], axis=0) for part in parts(experts)]
    others = [swap(group) for group in groups]
    square = square_of(rep, a_inverse)
    square = swap(square)
    *first, ps = early(rep, groups, tri, g_inverse, a_inverse, True)
    second = early(rep, others[:3], ps, g_inverse, a_inverse, False)
    a_factor, kept, u, part, xo, v, inv = products(rep, owner, others[3:], (first, second), ps, g_inverse, a_inverse)
    return a_factor, kept, finish(rep, square, part, xo, v, inv, u)


def slot_table(route_block, expert_count, capacity):
    top_k = route_block.shape[1]
    route_ids = route_block.reshape(-1)
    in_window = route_ids < expert_count
    columns = lax.broadcasted_iota(jnp.int32, (route_ids.shape[0], expert_count), 1)
    one_hot = ((route_ids[:, None] == columns) & in_window[:, None]).astype(jnp.int32)
    before = jnp.cumsum(one_hot, axis=0) - one_hot
    position = jnp.sum(before * one_hot, axis=1)
    sentinel = expert_count * capacity
    slot_ids = jnp.where(in_window, route_ids * capacity + position, sentinel)
    source_ids = jnp.arange(route_ids.shape[0], dtype=jnp.int32) // top_k
    slot_token = jnp.zeros((sentinel + 1,), jnp.int32).at[slot_ids].set(source_ids)
    filled = jnp.zeros((sentinel + 1,), jnp.int32).at[slot_ids].set(1)
    return (slot_token[:sentinel], filled[:sentinel])


def local_any(tokens, cotangents, routes, owner, a_inverse, g_inverse):
    expert_count = lax.axis_size("expert")
    replica_count = lax.axis_size("replica")
    width = tokens.shape[1]
    hidden_width = cotangents.shape[1]
    slot_token, filled = slot_table(routes, expert_count, CAP)
    slot_mask = filled.astype(jnp.bfloat16)[:, None]
    send_x = (jnp.take(tokens, slot_token, axis=0) * slot_mask).reshape(expert_count, CAP, width)
    send_y = (jnp.take(cotangents, slot_token, axis=0) * slot_mask).reshape(
        expert_count, CAP, hidden_width
    )
    sent_counts = jnp.sum(filled.reshape(expert_count, CAP), axis=1).astype(jnp.bfloat16)
    recv_x, recv_y, recv_counts = (
        lax.all_to_all(send_x, "expert", split_axis=0, concat_axis=0, tiled=True),
        lax.all_to_all(send_y, "expert", split_axis=0, concat_axis=0, tiled=True),
        lax.all_to_all(sent_counts, "expert", split_axis=0, concat_axis=0, tiled=True),
    )
    rows_x = recv_x.reshape(-1, width)
    rows_y = recv_y.reshape(-1, hidden_width)
    block_rows = width // replica_count
    own_start = lax.axis_index("replica") * block_rows
    piece_x = lax.all_gather(rows_x, "replica", axis=0, tiled=True)
    piece_y = lax.all_gather(rows_y, "replica", axis=0, tiled=True)
    piece_counts = lax.all_gather(recv_counts, "replica", axis=0, tiled=True)
    columns = lax.dynamic_slice_in_dim(piece_x, own_start, block_rows, 1)
    a_next = jnp.dot(columns.T, piece_x, preferred_element_type=jnp.float32)
    g_next = jnp.dot(piece_y.T, piece_y, preferred_element_type=jnp.float32)
    count_next = jnp.sum(piece_counts.astype(jnp.float32))
    mixed_own = jnp.dot(a_inverse[0], piece_x.T, preferred_element_type=jnp.float32).astype(BF16)
    mixed = lax.all_gather(mixed_own, "replica", axis=0, tiled=True)
    right = jnp.dot(piece_y, g_inverse[0], preferred_element_type=jnp.float32).astype(BF16)
    update = (jnp.dot(mixed, right, preferred_element_type=jnp.float32) / count_next).astype(BF16)
    a_factor = (a_next / count_next)[None]
    keeper = owner[0] == lax.axis_index("replica")
    kept = jnp.where(keeper, g_next / count_next, jnp.zeros_like(g_next))[None, None]
    return (a_factor, kept, update[None])


def solution(mesh):
    placed = (
        P(("expert", "replica"), None),
        P(("expert", "replica"), None),
        P(("expert", "replica"), None),
        P("expert"),
        P("expert", "replica", None),
        P("expert", None, None),
    )
    pair = mesh.shape["replica"] == 2
    return jax.shard_map(
        local if pair else local_any,
        mesh=mesh,
        in_specs=placed,
        out_specs=(
            P("expert", "replica", None),
            P("replica", "expert", None, None),
            P("expert", None, None),
        ),
        check_vma=False,
    )
```

```python
import functools

import jax
import jax.numpy as jnp
from jax import lax
from jax.experimental import pallas as pl
from jax.experimental.pallas import tpu as pltpu
from jax.sharding import PartitionSpec as P


CAP = 12
MAIN = 8
EMPTY = 1024.0

PAD = 8
TILE = 256
RING = 4
FOLD_VMEM = 50 * 2**20
AHEAD = 128


F32 = jnp.float32
BF16 = jnp.bfloat16
VMEM = pl.BlockSpec(memory_space=pltpu.VMEM)
SMEM = pl.BlockSpec(memory_space=pltpu.SMEM)
ANY = pl.BlockSpec(memory_space=pl.ANY)


def tiles(start, stop):
    return [(at, min(at + TILE, stop)) for at in range(start, stop, TILE)]


def dot(a, b):
    return jnp.dot(a, b, preferred_element_type=F32)


def dot_nt(a, b):
    return lax.dot_general(a, b, (((1,), (1,)), ((), ())), preferred_element_type=F32)


def dot_tn(a, b):
    return lax.dot_general(a, b, (((0,), (0,)), ((), ())), preferred_element_type=F32)


def target(me, block, experts):
    inner = experts // (2 * RING)
    place = (me // (2 * inner) + block // inner) % RING
    return (place * inner + (me // 2 % inner ^ block % inner)) * 2 + me % 2


def pack_kernel(me_ref, *refs):
    me = me_ref[0]
    sources, out_refs = (refs[0:3], refs[3:6]), refs[6:]
    top, toks = refs[0].shape
    width, hidden = refs[1].shape[1], refs[2].shape[1]
    half = (width + hidden) // 2
    base, split = width + hidden, width - half
    span = len(sources) * MAIN
    rows = len(out_refs) * span
    row = lax.broadcasted_iota(jnp.int32, (rows, toks), 0)
    ids = target(me, row // span, 2 * len(out_refs))
    sub = row % MAIN
    low = sub < MAIN // 2
    earlier = lax.broadcasted_iota(jnp.int32, (toks, toks), 0) < lax.broadcasted_iota(
        jnp.int32, (toks, toks), 1
    )
    earlier = jnp.where(earlier, 1.0, 0.0).astype(BF16)
    picks, lows, highs = [], [], []
    full, full_rest = 0.0, 0.0
    for n, (routes_ref, _, _) in enumerate(sources):
        mine = row // MAIN % len(sources) == n
        chosen = jnp.zeros((rows, toks), F32)
        for k in range(top):
            chosen += jnp.where((routes_ref[k : k + 1, :] == ids) & mine, 1.0, 0.0)
        slot = jnp.where(chosen > 0.0, dot(chosen.astype(BF16), earlier), -1.0).astype(jnp.int32)
        pick = jnp.where(slot == sub, 1.0, 0.0)
        rest = jnp.where(slot == jnp.where(low, MAIN + sub, MAIN // 2 + sub), 1.0, 0.0)
        full += jnp.sum(pick, axis=1, keepdims=True)
        full_rest += jnp.sum(rest, axis=1, keepdims=True)
        picks.append(pick.astype(BF16))
        lows.append(jnp.where(low, rest, 0.0).astype(BF16))
        highs.append(jnp.where(low, 0.0, rest).astype(BF16))
    lane0 = lax.broadcasted_iota(jnp.int32, (rows, 128), 1) == 0
    low_lanes = lax.broadcasted_iota(jnp.int32, (rows, 128), 0) % MAIN < MAIN // 2

    def put(at, value):
        for q, ref in enumerate(out_refs):
            ref[:, at : at + value.shape[1]] = value[q * span : (q + 1) * span].astype(BF16)

    def x(which, cols):
        return sum(dot(w, refs[cols]) for w, (_, refs, _) in zip(which, sources))

    def y(which):
        return sum(dot(w, ref[...]) for w, (_, _, ref) in zip(which, sources))

    first = x(picks, (slice(None), slice(0, 128)))
    put(0, jnp.where(lane0 & (full == 0.0), EMPTY, first))
    put(128, x(picks, (slice(None), slice(128, width))))
    put(width, y(picks))
    rem = x(lows, (slice(None), slice(0, split))) + x(highs, (slice(None), slice(half, width)))
    put(base, jnp.where(lane0 & low_lanes & (full_rest == 0.0), EMPTY, rem[:, :128]))
    put(base + 128, rem[:, 128:])
    put(base + split, x(lows, (slice(None), slice(split, half))) + y(highs))


def pack(me, mine, other, blocks):
    toks, width = mine[1].shape
    width = (width + mine[2].shape[1]) * CAP // MAIN
    return pl.pallas_call(
        pack_kernel,
        name="pack",
        out_shape=[jax.ShapeDtypeStruct((2 * MAIN, width), BF16)] * blocks,
        in_specs=[SMEM] + [VMEM] * 6,
        out_specs=[VMEM] * blocks,
        compiler_params=pltpu.CompilerParams(vmem_limit_bytes=12 * 2**20),
        cost_estimate=pl.CostEstimate(
            flops=8 * blocks * MAIN * toks * width, bytes_accessed=3 * 2**20, transcendentals=0
        ),
    )(me, *mine, *other)


def fold_kernel(rep_ref, a_hbm, out_ref, p_ref, s_ref, sems):
    half = p_ref.shape[0]
    at = pl.multiple_of(rep_ref[0] * 2 * half, 2 * half)
    step = half // 4
    loads = []
    for top in range(0, half, step):
        for ref, down, over in ((p_ref, 0, 0), (s_ref, half, half)):
            src = a_hbm.at[0, pl.ds(down + top, step), pl.ds(at + over, half)]
            loads.append(pltpu.make_async_copy(src, ref.at[pl.ds(top, step)], sems.at[len(loads)]))
    if AHEAD:
        src = a_hbm.at[0, pl.ds(0, AHEAD), pl.ds(at + half, half)]
        loads.append(pltpu.make_async_copy(src, out_ref.at[pl.ds(half + PAD, AHEAD)], sems.at[len(loads)]))
    for load in loads:
        load.start()
    row = lax.broadcasted_iota(jnp.int32, (half, half), 0)
    col = lax.broadcasted_iota(jnp.int32, (half, half), 1)
    for load in loads:
        load.wait()
    p, s = p_ref[...].astype(F32), s_ref[...].astype(F32)
    out_ref[:half, :] = jnp.where(col >= row, p, s).astype(BF16)
    diagonal = jnp.sum(jnp.where(row == col, s, 0.0), axis=0, keepdims=True)
    out_ref[half : half + PAD, :] = jnp.broadcast_to(diagonal, (PAD, half)).astype(BF16)


def fold(rep, a_inverse):
    half = a_inverse.shape[1] // 2
    rows = half + PAD + AHEAD
    return pl.pallas_call(
        fold_kernel,
        name="fold",
        out_shape=jax.ShapeDtypeStruct((rows, half), BF16),
        in_specs=[SMEM, ANY],
        out_specs=VMEM,
        scratch_shapes=[
            pltpu.VMEM((half, half), BF16),
            pltpu.VMEM((half, half), BF16),
            pltpu.SemaphoreType.DMA((9,)),
        ],
        compiler_params=pltpu.CompilerParams(vmem_limit_bytes=FOLD_VMEM),
        cost_estimate=pl.CostEstimate(flops=half * half, bytes_accessed=6 * half * half, transcendentals=0),
    )(rep, a_inverse)


def square_kernel(rep_ref, q_ref, out_ref):
    out_ref[...] = q_ref[0, AHEAD:, :]


def square_of(rep, a_inverse):
    half = a_inverse.shape[1] // 2
    return pl.pallas_call(
        square_kernel,
        name="square",
        out_shape=jax.ShapeDtypeStruct((half - AHEAD, half), BF16),
        grid_spec=pltpu.PrefetchScalarGridSpec(
            num_scalar_prefetch=1,
            grid=(1,),
            in_specs=[pl.BlockSpec((1, half, half), lambda i, rep: (0, 0, 2 * rep[0] + 1))],
            out_specs=pl.BlockSpec((half - AHEAD, half), lambda i, rep: (0, 0)),
        ),
        compiler_params=pltpu.CompilerParams(vmem_limit_bytes=6 * 2**20),
        cost_estimate=pl.CostEstimate(flops=half * half, bytes_accessed=2 * half * half, transcendentals=0),
    )(rep, a_inverse)


def gather_rows(groups, x_ref, y_ref, at):
    cols = x_ref.shape[2]
    width = 2 * cols
    hidden = y_ref.shape[1]
    half = (width + hidden) // 2
    base = width + hidden
    start = at
    for ref in groups:
        count = ref.shape[0]
        x_ref[0, at : at + count, :] = ref[:, :cols]
        x_ref[1, at : at + count, :] = ref[:, cols:width]
        y_ref[at : at + count, :] = ref[:, width:base]
        at += count
    for ref in groups:
        count = ref.shape[0] // 2
        low = lax.broadcasted_iota(jnp.int32, (count, half), 0) % MAIN < MAIN // 2
        one, two = ref[:count, base:].astype(F32), ref[count:, base:].astype(F32)
        lo = jnp.where(low, one, pltpu.roll(two, MAIN // 2, 0)).astype(BF16)
        hi = jnp.where(low, pltpu.roll(one, count - MAIN // 2, 0), two).astype(BF16)
        x_ref[0, at : at + count, :] = lo[:, :cols]
        x_ref[1, at : at + count, : half - cols] = lo[:, cols:]
        x_ref[1, at : at + count, half - cols :] = hi[:, : width - half]
        y_ref[at : at + count, :] = hi[:, width - half :]
        at += count
    edge = x_ref[0, start:at, :128].astype(F32)
    empty = (lax.broadcasted_iota(jnp.int32, edge.shape, 1) == 0) & (edge == EMPTY)
    x_ref[0, start:at, :128] = jnp.where(empty, 0.0, edge).astype(BF16)
    return (at - start) - jnp.sum(jnp.where(empty, 1.0, 0.0))


def mix_rows(x_ref, rows, a_ref, ps_ref, rep, own_ref, part_ref):
    oth = 1 - rep
    side = x_ref.shape[2]
    half = side // 2
    own_at, oth_at = pl.multiple_of(rep * side, side), pl.multiple_of(oth * side, side)
    x_own, x_oth = x_ref[rep, rows, :], x_ref[oth, rows, :]
    for c in range(side // TILE):
        cols = slice(c * TILE, (c + 1) * TILE)
        own_ref[rows, cols] = (
            dot(x_own, a_ref[0, :, pl.ds(own_at + c * TILE, TILE)])
            + dot_nt(x_oth, a_ref[0, cols, pl.ds(oth_at, side)])
        ).astype(BF16)
    for c in range(side // TILE):
        h, inner = divmod(c * TILE, half)
        value = dot(x_own, a_ref[0, :, pl.ds(oth_at + c * TILE, TILE)]) + dot(
            x_oth[:, h * half : (h + 1) * half], ps_ref[h, :, inner : inner + TILE]
        )
        if h == 1 and AHEAD:
            value += dot(x_oth[:, :AHEAD], ps_ref[2, :AHEAD, inner : inner + TILE])
        ready = min(max(AHEAD - c * TILE, 0), TILE)
        if ready:
            full = value[:, :ready] + dot_nt(x_oth[:, half:], ps_ref[2, inner : inner + ready, :])
            own_ref[rows, side + c * TILE : side + c * TILE + ready] = full.astype(BF16)
        if ready < TILE:
            part_ref[rows, c * TILE + ready - AHEAD : (c + 1) * TILE - AHEAD] = value[:, ready:]


def early_kernel(rep_ref, *refs, groups, unfold):
    blocks = refs[:groups]
    tri_ref, g_ref, a_ref, x_ref, y_ref, own_ref, part_ref, v_ref, count_ref = refs[groups : groups + 9]
    ps_ref = refs[-1]
    rep = rep_ref[0]
    half = tri_ref.shape[1]
    if unfold:
        if AHEAD:
            ps_ref[2, :AHEAD, :] = tri_ref[half + PAD :, :]
        mix = tri_ref[:half, :].astype(F32)
        mix_t = mix.T
        row = lax.broadcasted_iota(jnp.int32, (half, half), 0)
        col = lax.broadcasted_iota(jnp.int32, (half, half), 1)
        diagonal = tri_ref[half : half + 1, :].astype(F32)
        ps_ref[0] = jnp.where(col >= row, mix, mix_t).astype(BF16)
        ps_ref[1] = jnp.where(col < row, mix, jnp.where(col == row, diagonal, mix_t)).astype(BF16)
    else:
        ps_ref = tri_ref
    count = gather_rows(blocks, x_ref, y_ref, 0)
    count_ref[...] = jnp.full(count_ref.shape, count, F32)
    v_ref[...] = dot(y_ref[...], g_ref[0]).astype(BF16)
    mix_rows(x_ref, slice(0, x_ref.shape[1]), a_ref, ps_ref, rep, own_ref, part_ref)


def early(rep, groups, tri, g_inverse, a_inverse, unfold):
    rows = sum(g.shape[0] for g in groups) * CAP // MAIN
    _, side, width = a_inverse.shape
    hidden = g_inverse.shape[1]
    half = side // 2
    tri_shape = [jax.ShapeDtypeStruct((3 if AHEAD else 2, half, half), BF16)] if unfold else []
    return pl.pallas_call(
        functools.partial(early_kernel, groups=len(groups), unfold=unfold),
        name="early",
        out_shape=[
            jax.ShapeDtypeStruct((2, rows, side), BF16),
            jax.ShapeDtypeStruct((rows, hidden), BF16),
            jax.ShapeDtypeStruct((rows, side + AHEAD), BF16),
            jax.ShapeDtypeStruct((rows, side - AHEAD), F32),
            jax.ShapeDtypeStruct((rows, hidden), BF16),
            jax.ShapeDtypeStruct((8, 128), F32),
        ]
        + tri_shape,
        in_specs=[SMEM] + [VMEM] * (len(groups) + 3),
        out_specs=[VMEM] * (6 + unfold),
        compiler_params=pltpu.CompilerParams(vmem_limit_bytes=20 * 2**20),
        cost_estimate=pl.CostEstimate(flops=4 * rows * width * side, bytes_accessed=2**23, transcendentals=0),
    )(rep, *groups, tri, g_inverse, a_inverse)


def main_kernel(rep_ref, owner_ref, *refs, groups, bundles):
    blocks = refs[:groups]
    done = [refs[groups + 6 * n : groups + 6 * (n + 1)] for n in range(bundles)]
    (
        ps_ref, g_ref, a_ref,
        a_out, kept_out, u_out, part_ref, xo_ref, v_ref, inv_ref,
        x_ref, y_ref, own_ref, abuf, gbuf, ubuf, a_sem, g_sem, u_sem,
    ) = refs[groups + 6 * bundles :]
    rep = rep_ref[0]
    oth = 1 - rep
    side = x_ref.shape[2]
    at = 0
    count = 0.0
    for x_in, y_in, own_in, part_in, v_in, count_in in done:
        more = at + y_in.shape[0]
        x_ref[:, at:more, :] = x_in[...]
        y_ref[at:more, :] = y_in[...]
        own_ref[at:more, :] = own_in[...]
        part_ref[at:more, :] = part_in[...]
        v_ref[at:more, :] = v_in[...]
        count = count + count_in[...]
        at = more
    count = count + gather_rows(blocks, x_ref, y_ref, at)
    v_ref[at:, :] = dot(y_ref[at:, :], g_ref[0]).astype(BF16)
    mix_rows(x_ref, slice(at, x_ref.shape[1]), a_ref, ps_ref, rep, own_ref, part_ref)
    inv = 1.0 / count
    inv_ref[...] = inv
    inv = inv[:1, :1]

    writes = []
    for i in range(side // TILE):
        lhs = x_ref[rep, :, i * TILE : (i + 1) * TILE]
        for h in range(2):
            abuf[i, :, h * side : (h + 1) * side] = dot_tn(lhs, x_ref[h]) * inv
        write = pltpu.make_async_copy(abuf.at[i], a_out.at[0, pl.ds(i * TILE, TILE), :], a_sem.at[i])
        write.start()
        writes.append(write)

    keep = jnp.where(owner_ref[0] == rep, 1.0, 0.0) * inv
    gbuf[...] = dot_tn(y_ref[...], y_ref[...]) * keep
    write = pltpu.make_async_copy(gbuf, kept_out.at[0, 0], g_sem)
    write.start()
    writes.append(write)

    xo_ref[...] = x_ref[oth, :, AHEAD:]
    for n, (c0, c1) in enumerate([(0, side // 2), (side // 2, side)] + tiles(side, side + AHEAD)):
        ubuf[c0:c1, :] = (dot_tn(own_ref[:, c0:c1], v_ref[...]) * inv).astype(BF16)
        to = rep * side + c0 if c0 < side else oth * side + c0 - side
        write = pltpu.make_async_copy(
            ubuf.at[pl.ds(c0, c1 - c0)], u_out.at[0, pl.ds(to, c1 - c0), :], u_sem.at[n]
        )
        write.start()
        writes.append(write)
    for write in writes:
        write.wait()


def products(rep, owner, groups, done, ps, g_inverse, a_inverse):
    rows = sum(d[1].shape[0] for d in done) + sum(g.shape[0] for g in groups) * CAP // MAIN
    _, side, width = a_inverse.shape
    hidden = g_inverse.shape[1]
    return pl.pallas_call(
        functools.partial(main_kernel, groups=len(groups), bundles=len(done)),
        name="products",
        out_shape=[
            jax.ShapeDtypeStruct((1, side, width), F32),
            jax.ShapeDtypeStruct((1, 1, hidden, hidden), F32),
            jax.ShapeDtypeStruct((1, width, hidden), BF16),
            jax.ShapeDtypeStruct((rows, side - AHEAD), F32),
            jax.ShapeDtypeStruct((rows, side - AHEAD), BF16),
            jax.ShapeDtypeStruct((rows, hidden), BF16),
            jax.ShapeDtypeStruct((8, 128), F32),
        ],
        in_specs=[SMEM, SMEM] + [VMEM] * (len(groups) + 6 * len(done) + 3),
        out_specs=[ANY, ANY, ANY, VMEM, VMEM, VMEM, VMEM],
        scratch_shapes=[
            pltpu.VMEM((2, rows, side), BF16),
            pltpu.VMEM((rows, hidden), BF16),
            pltpu.VMEM((rows, side + AHEAD), BF16),
            pltpu.VMEM((side // TILE, TILE, width), F32),
            pltpu.VMEM((hidden, hidden), F32),
            pltpu.VMEM((side + AHEAD, hidden), BF16),
            pltpu.SemaphoreType.DMA((side // TILE,)),
            pltpu.SemaphoreType.DMA,
            pltpu.SemaphoreType.DMA((len(tiles(0, side) + tiles(side, side + AHEAD)),)),
        ],
        compiler_params=pltpu.CompilerParams(vmem_limit_bytes=36 * 2**20),
        cost_estimate=pl.CostEstimate(
            flops=4 * rows * width * side, bytes_accessed=12 * 2**20, transcendentals=0
        ),
    )(rep, owner, *groups, *[value for d in done for value in d], ps, g_inverse, a_inverse)


def last_kernel(rep_ref, square_ref, part_ref, x_ref, v_ref, inv_ref, u_in, u_out, ubuf, u_sem):
    oth = 1 - rep_ref[0]
    rest, half = square_ref.shape
    side = 2 * half
    inv = inv_ref[:1, :1]
    stores = []
    for n, (c0, c1) in enumerate([(rest, rest + half), (0, rest)]):
        if c0 < rest:
            extra = dot_nt(x_ref[:, rest:], square_ref[c0:c1, :])
        else:
            extra = dot(x_ref[:, :rest], square_ref[:, c0 - rest : c1 - rest])
        mixed = (part_ref[:, c0:c1] + extra).astype(BF16)
        ubuf[c0:c1, :] = (dot_tn(mixed, v_ref[...]) * inv).astype(BF16)
        store = pltpu.make_async_copy(
            ubuf.at[pl.ds(c0, c1 - c0)],
            u_out.at[0, pl.ds(oth * side + half - rest + c0, c1 - c0), :],
            u_sem.at[n],
        )
        store.start()
        stores.append(store)
    for store in stores:
        store.wait()


def finish(rep, square, part, x, v, inv, u):
    side, hidden = part.shape[1], v.shape[1]
    return pl.pallas_call(
        last_kernel,
        name="finish",
        out_shape=jax.ShapeDtypeStruct(u.shape, BF16),
        in_specs=[SMEM] + [VMEM] * 5 + [ANY],
        out_specs=ANY,
        input_output_aliases={6: 0},
        scratch_shapes=[
            pltpu.VMEM((side, hidden), BF16),
            pltpu.SemaphoreType.DMA((2,)),
        ],
        compiler_params=pltpu.CompilerParams(vmem_limit_bytes=16 * 2**20),
        cost_estimate=pl.CostEstimate(
            flops=2 * part.shape[0] * side * (side + hidden), bytes_accessed=4 * 2**20, transcendentals=0
        ),
    )(rep, square, part, x, v, inv, u)


def parts(experts):
    inner = experts // (2 * RING)
    half = inner // 2
    return [
        list(range(inner)),
        [s * inner + w for s in (1, 3) for w in range(half)],
        [s * inner + w for s in (1, 3) for w in range(half, inner)],
        list(range(2 * inner, 3 * inner)),
    ]


def local(tokens, cotangents, routes, owner, a_inverse, g_inverse):
    experts = lax.axis_size("expert")
    me = lax.axis_index("expert").astype(jnp.int32).reshape(1)
    rep = lax.axis_index("replica").astype(jnp.int32).reshape(1)

    def swap(value):
        return lax.ppermute(value, "replica", [(0, 1), (1, 0)])

    def trade(value, to):
        return lax.ppermute(value, "expert", [(i, to(i)) for i in range(experts)])

    tri = fold(rep, a_inverse)
    tri = swap(tri)
    mine = (routes.T, tokens, cotangents)
    other = tuple(trade(value, lambda i: i ^ 1) for value in mine)
    blocks = pack(me, mine, other, experts // 2)
    got = [blocks[0]]
    for q in range(1, experts // 2):
        got.append(trade(blocks[q], lambda i, q=q: target(i, q, experts)))
    groups = [jnp.concatenate([got[q] for q in part], axis=0) for part in parts(experts)]
    others = [swap(group) for group in groups]
    square = square_of(rep, a_inverse)
    square = swap(square)
    *first, ps = early(rep, groups, tri, g_inverse, a_inverse, True)
    second = early(rep, others[:3], ps, g_inverse, a_inverse, False)
    a_factor, kept, u, part, xo, v, inv = products(rep, owner, others[3:], (first, second), ps, g_inverse, a_inverse)
    return a_factor, kept, finish(rep, square, part, xo, v, inv, u)


def slot_table(route_block, expert_count, capacity):
    top_k = route_block.shape[1]
    route_ids = route_block.reshape(-1)
    in_window = route_ids < expert_count
    columns = lax.broadcasted_iota(jnp.int32, (route_ids.shape[0], expert_count), 1)
    one_hot = ((route_ids[:, None] == columns) & in_window[:, None]).astype(jnp.int32)
    before = jnp.cumsum(one_hot, axis=0) - one_hot
    position = jnp.sum(before * one_hot, axis=1)
    sentinel = expert_count * capacity
    slot_ids = jnp.where(in_window, route_ids * capacity + position, sentinel)
    source_ids = jnp.arange(route_ids.shape[0], dtype=jnp.int32) // top_k
    slot_token = jnp.zeros((sentinel + 1,), jnp.int32).at[slot_ids].set(source_ids)
    filled = jnp.zeros((sentinel + 1,), jnp.int32).at[slot_ids].set(1)
    return (slot_token[:sentinel], filled[:sentinel])


def local_any(tokens, cotangents, routes, owner, a_inverse, g_inverse):
    expert_count = lax.axis_size("expert")
    replica_count = lax.axis_size("replica")
    width = tokens.shape[1]
    hidden_width = cotangents.shape[1]
    slot_token, filled = slot_table(routes, expert_count, CAP)
    slot_mask = filled.astype(jnp.bfloat16)[:, None]
    send_x = (jnp.take(tokens, slot_token, axis=0) * slot_mask).reshape(expert_count, CAP, width)
    send_y = (jnp.take(cotangents, slot_token, axis=0) * slot_mask).reshape(
        expert_count, CAP, hidden_width
    )
    sent_counts = jnp.sum(filled.reshape(expert_count, CAP), axis=1).astype(jnp.bfloat16)
    recv_x, recv_y, recv_counts = (
        lax.all_to_all(send_x, "expert", split_axis=0, concat_axis=0, tiled=True),
        lax.all_to_all(send_y, "expert", split_axis=0, concat_axis=0, tiled=True),
        lax.all_to_all(sent_counts, "expert", split_axis=0, concat_axis=0, tiled=True),
    )
    rows_x = recv_x.reshape(-1, width)
    rows_y = recv_y.reshape(-1, hidden_width)
    block_rows = width // replica_count
    own_start = lax.axis_index("replica") * block_rows
    piece_x = lax.all_gather(rows_x, "replica", axis=0, tiled=True)
    piece_y = lax.all_gather(rows_y, "replica", axis=0, tiled=True)
    piece_counts = lax.all_gather(recv_counts, "replica", axis=0, tiled=True)
    columns = lax.dynamic_slice_in_dim(piece_x, own_start, block_rows, 1)
    a_next = jnp.dot(columns.T, piece_x, preferred_element_type=jnp.float32)
    g_next = jnp.dot(piece_y.T, piece_y, preferred_element_type=jnp.float32)
    count_next = jnp.sum(piece_counts.astype(jnp.float32))
    mixed_own = jnp.dot(a_inverse[0], piece_x.T, preferred_element_type=jnp.float32).astype(BF16)
    mixed = lax.all_gather(mixed_own, "replica", axis=0, tiled=True)
    right = jnp.dot(piece_y, g_inverse[0], preferred_element_type=jnp.float32).astype(BF16)
    update = (jnp.dot(mixed, right, preferred_element_type=jnp.float32) / count_next).astype(BF16)
    a_factor = (a_next / count_next)[None]
    keeper = owner[0] == lax.axis_index("replica")
    kept = jnp.where(keeper, g_next / count_next, jnp.zeros_like(g_next))[None, None]
    return (a_factor, kept, update[None])


def solution(mesh):
    placed = (
        P(("expert", "replica"), None),
        P(("expert", "replica"), None),
        P(("expert", "replica"), None),
        P("expert"),
        P("expert", "replica", None),
        P("expert", None, None),
    )
    pair = mesh.shape["replica"] == 2
    return jax.shard_map(
        local if pair else local_any,
        mesh=mesh,
        in_specs=placed,
        out_specs=(
            P("expert", "replica", None),
            P("replica", "expert", None, None),
            P("expert", None, None),
        ),
        check_vma=False,
    )
```
